512 devices in a mesh: groups: 2 (over y), slab: 32 (over z), coil: 4 (over x), row: 2 (over core).
Axes of the slice: x: 4, y: 2, z: 32, core: 2. Of those that a mesh axis runs over, the one named last changes fastest.
The devices are a block of a 4x16x32 slice.
Arguments:
- image: float32 [4, 128, 256, 128], P('groups', None, ('slab', 'row')), parts along dimension 0, may hold values from -6 to 6
- sens: bfloat16 [4, 16, 128, 256, 128], P('groups', 'coil', None, ('slab', 'row')), parts along dimension 0, may hold values from -1.5 to 1.5
- measured: bfloat16 [4, 16, 128, 256, 128], P('groups', 'coil', ('slab', 'row')), parts along dimension 0, may hold values from -3 to 3
- mask: int32 [128, 256], P(('slab', 'row')), may hold values from 0 to 1, as said below
- thresholds: float32 [2, 7], replicated, may hold values from 0.1 to 1.5
Outputs:
- image_next: float32 [4, 128, 256, 128], P('groups', None, ('slab', 'row')), parts along dimension 0
The draws below stay inside these ranges and needn't reach their ends.
There are 2 independent parts, one for each index of `groups`. The reference program is written for one: setup_inputs(seed, part) draws one part's arguments, and reference() takes and returns one part's arrays. A program takes and returns all parts, laid end to end along the dimension named above; an argument that names none is the same for every part. Nothing has to cross between parts.
Inputs may be any that keep to these rules, and one draw needn't show every extreme that they name: `mask`: A calibration block of the 8 central phase-encode lines (ky from 60 to 67) is sampled at every kz; outside it each (ky, kz) is sampled independently at random.
All inputs are finite; a program needn't handle non-finite values.
Results may differ from the reference program's by a relative error of at most 0.013.
Values may be sent and summed in bfloat16 or wider, within the bound.
No kernel may reach another device: no remote copies, remote signals or barrier semaphores. Data moves between devices by JAX's collectives and lax.ppermute only.
A program may use at most 128 MiB of HBM per device.

```python
import math
import jax
import jax.numpy as jnp
from jax import lax

X = 128
Y = 128
Z = 256
C = 16
LEVELS = 2


def draw_mask(key, part):
    drawn = jax.random.randint(key, (Y, Z), 0, 3)
    scattered = (drawn == 0).astype(jnp.int32)
    line_index = jnp.arange(Y, dtype=jnp.int32)[:, None]
    calibration = ((line_index >= Y // 2 - 4) & (line_index < Y // 2 + 4)).astype(jnp.int32)
    return jnp.maximum(scattered, jnp.broadcast_to(calibration, (Y, Z)))


def steps_of(key, extent, split, least, top_value):
    gain = 1.0
    for position, blocks in split:
        steps = jax.random.uniform(jax.random.fold_in(jax.random.fold_in(key, 6), position), (blocks,), jnp.float32, least / len(split), top_value / len(split))
        gain = gain * jnp.repeat(jnp.exp(steps), extent[position] // blocks).reshape((-1,) + (1,) * (len(extent) - 1 - position))
    return gain


def noise(stream_key, extent, width, bound, cuts=(), kind=jnp.bfloat16):
    result = width * jax.random.normal(stream_key, extent, jnp.float32)
    if cuts:
        result = result * steps_of(stream_key, extent, cuts, -0.22, 0.18)
    return jnp.clip(result, -bound, bound).astype(kind)


def setup_inputs(seed: int = 0, part: int = 0) -> dict:
    seeds = jax.random.split(jax.random.key(seed), 6)
    own_keys = jax.random.split(jax.random.fold_in(seeds[5], part), 6)
    image = noise(own_keys[0], (2, Y, Z, X), 1.0, 6.0, ((2, 64),), jnp.float32)
    sens = noise(own_keys[1], (2, C, Y, Z, X), 0.25, 1.5, ((1, 4), (3, 64)))
    measured = noise(own_keys[2], (2, C, Y, Z, X), 0.5, 3.0, ((1, 4), (2, 64)))
    mask = draw_mask(jax.random.fold_in(seeds[5], 71), part)
    thresholds = jnp.clip(jnp.exp(jax.random.uniform(seeds[4], (LEVELS, 7), jnp.float32, math.log(0.1), math.log(1.5))), 0.1, 1.5)
    return {"image": image, "sens": sens, "measured": measured, "mask": mask, "thresholds": thresholds}


half_root = 0.7071067811865476
quarter_root = 0.3535533905932738
step_size = 0.5

def fourier_table(length, sign):
    index = jnp.arange(length, dtype=jnp.int32)
    phase = index[:, None] * index[None, :] % length
    theta = phase.astype(jnp.float32) * jnp.float32(2.0 * math.pi / length)
    scale = jnp.float32(1.0 / math.sqrt(length))
    real = jnp.cos(theta) * scale
    imaginary = jnp.sin(theta) * (sign * scale)
    upper = jnp.stack([real, -imaginary])
    lower = jnp.stack([imaginary, real])
    return jnp.stack([upper, lower]).astype(jnp.bfloat16)

def contract(form, values, table):
    return jnp.einsum(form, values.astype(jnp.float32), table.astype(jnp.float32), precision=lax.Precision.HIGHEST)

def complex_product(left, right):
    return jnp.stack([left[0] * right[0] - left[1] * right[1], left[0] * right[1] + left[1] * right[0]])

def roll_after(values, along, offset):
    return jnp.roll(values, -offset, axis=along)

def roll_before(values, along, offset):
    return jnp.roll(values, offset, axis=along)

def split_bands(bands, along, offset, after):
    moved = after(bands, along, offset)
    return jnp.concatenate([(bands + moved) * half_root, (bands - moved) * half_root], axis=0)

def merge_bands(bands, along, offset, before):
    half = bands.shape[0] // 2
    lower = bands[:half]
    upper = bands[half:]
    return (lower + upper + before(lower - upper, along, offset)) * quarter_root

def shrink_detail(detail, limit):
    magnitude = jnp.sqrt(detail[:, 0] * detail[:, 0] + detail[:, 1] * detail[:, 1])
    limit = limit.reshape((-1, 1, 1, 1))
    factor = jnp.maximum(magnitude - limit, 0.0) / jnp.maximum(magnitude, limit)
    return detail * factor[:, None]

def wavelet_shrink(descent, thresholds, moves):
    coarse = descent[None]
    details = []
    for level in range(thresholds.shape[0]):
        offset = 2 ** level
        bands = coarse
        for along, after, before in moves:
            bands = split_bands(bands, along, offset, after)
        coarse = bands[:1]
        details.append(shrink_detail(bands[1:], thresholds[level]))
    for level in reversed(range(thresholds.shape[0])):
        offset = 2 ** level
        bands = jnp.concatenate([coarse, details[level]], axis=0)
        for along, after, before in reversed(moves):
            bands = merge_bands(bands, along, offset, before)
        coarse = bands
    return coarse[0]

def reference(image, sens, measured, mask, thresholds):
    table_readout = fourier_table(image.shape[3], -1.0)
    table_phase = fourier_table(image.shape[1], -1.0)
    table_depth = fourier_table(image.shape[2], -1.0)
    inverse_readout = fourier_table(image.shape[3], 1.0)
    inverse_phase = fourier_table(image.shape[1], 1.0)
    inverse_depth = fourier_table(image.shape[2], 1.0)
    sampled = mask.astype(jnp.float32)[None, :, :, None]

    def coil_step(total, pieces):
        coil_sens, coil_data = pieces
        sens_wide = coil_sens.astype(jnp.float32)
        coil_image = complex_product(sens_wide, image).astype(jnp.bfloat16)
        readout_done = contract('tyzj,stjk->syzk', coil_image, table_readout).astype(jnp.bfloat16)
        phase_done = contract('tjzx,stjk->skzx', readout_done, table_phase).astype(jnp.bfloat16)
        spectrum = contract('tyjx,stjk->sykx', phase_done, table_depth)
        residual = (sampled * (spectrum - coil_data.astype(jnp.float32))).astype(jnp.bfloat16)
        depth_back = contract('tyjx,stjk->sykx', residual, inverse_depth).astype(jnp.bfloat16)
        phase_back = contract('tjzx,stjk->skzx', depth_back, inverse_phase).astype(jnp.bfloat16)
        readout_back = contract('tyzj,stjk->syzk', phase_back, inverse_readout)
        term = jnp.stack([sens_wide[0] * readout_back[0] + sens_wide[1] * readout_back[1], sens_wide[0] * readout_back[1] - sens_wide[1] * readout_back[0]])
        return (total + term, None)
    gradient, _ = lax.scan(coil_step, jnp.zeros(image.shape, jnp.float32), (jnp.moveaxis(sens, 1, 0), jnp.moveaxis(measured, 1, 0)))
    descent = image - step_size * gradient
    moves = [(4, roll_after, roll_before), (2, roll_after, roll_before), (3, roll_after, roll_before)]
    return wavelet_shrink(descent, thresholds, moves)
```

```python
import math

import jax
import jax.numpy as jnp
import ml_dtypes
import numpy as np
from jax import lax
from jax.experimental import pallas as pl
from jax.experimental.pallas import tpu as pltpu
from jax.sharding import PartitionSpec as P

step_size = 0.5
lines_axes = ("slab", "row")
chunk_count = 1


def fourier_table(length, sign, rows=None, columns=None):
    index = np.arange(length, dtype=np.int64)
    phase = (index[:, None] * index[None, :]) % length
    theta = phase.astype(np.float32) * np.float32(2.0 * math.pi / length)
    scale = np.float32(1.0 / math.sqrt(length))
    real = (np.cos(theta) * scale).astype(np.float32)
    imaginary = (np.sin(theta) * np.float32(sign) * scale).astype(np.float32)
    if rows is not None:
        real, imaginary = real[rows], imaginary[rows]
    if columns is not None:
        real, imaginary = real[:, columns], imaginary[:, columns]
    return np.block([[real, -imaginary], [imaginary, real]]).astype(ml_dtypes.bfloat16)


def dot(left, right):
    return jnp.dot(left, right, preferred_element_type=jnp.float32)


def forward_kernel(devices, lines, planes, sens_ref, image_ref, table_ref, out_ref, product, mixed):
    cells = product.shape[1] // planes
    group = lines * planes
    sr = sens_ref[0, 0].astype(jnp.float32)
    si = sens_ref[1, 0].astype(jnp.float32)
    ir = image_ref[0]
    ii = image_ref[1]
    product[0] = sr * ir - si * ii
    product[1] = sr * ii + si * ir
    columns = [
        jnp.concatenate(
            [product[t, pl.ds(z, cells, stride=planes), :].astype(jnp.bfloat16) for t in range(2)],
            axis=0,
        )
        for z in range(planes)
    ]
    done = dot(table_ref[...], jnp.concatenate(columns, axis=1))
    width = product.shape[2]
    for s in range(2):
        for z in range(planes):
            for line in range(lines):
                first = s * cells + line * devices
                mixed[s, pl.ds(z * lines + line, devices, stride=group), :] = done[
                    first : first + devices, z * width : (z + 1) * width
                ]
        out_ref[:, s, 0] = mixed[s].astype(jnp.bfloat16).reshape(devices, group, width)


def middle_kernel(lines, in_ref, measured_ref, mask_ref, table_ref, inverse_ref, out_ref, mixed, back):
    devices, _, _, group, width = in_ref.shape
    cells = devices * group // lines
    for t in range(2):
        mixed[t] = in_ref[:, t, 0].astype(jnp.float32).reshape(devices * group, width)
    columns = [
        jnp.concatenate(
            [mixed[t, pl.ds(line, cells, stride=lines), :].astype(jnp.bfloat16) for t in range(2)],
            axis=0,
        )
        for line in range(lines)
    ]
    spectrum = dot(table_ref[...], jnp.concatenate(columns, axis=1))
    residual = []
    for line in range(lines):
        parts = []
        for t in range(2):
            value = spectrum[t * cells : (t + 1) * cells, line * width : (line + 1) * width]
            value = mask_ref[line] * (value - measured_ref[t, 0, line].astype(jnp.float32))
            parts.append(value.astype(jnp.bfloat16))
        residual.append(jnp.concatenate(parts, axis=0))
    result = dot(inverse_ref[...], jnp.concatenate(residual, axis=1))
    for s in range(2):
        for line in range(lines):
            back[s, pl.ds(line, cells, stride=lines), :] = result[
                s * cells : (s + 1) * cells, line * width : (line + 1) * width
            ]
        out_ref[:, s, 0] = back[s].astype(jnp.bfloat16).reshape(devices, group, width)


def backward_kernel(lines, planes, first_ref, in_ref, sens_ref, table_ref, out_ref, mixed, wide, total):
    devices, _, _, group, width = in_ref.shape
    cells = devices * lines
    coil = pl.program_id(0)

    @pl.when(coil == 0)
    def _():
        if first_ref is None:
            total[...] = jnp.zeros(total.shape, jnp.float32)
        else:
            total[...] = first_ref[...]

    for t in range(2):
        mixed[t] = in_ref[:, t, 0].astype(jnp.float32).reshape(devices * group, width)
        wide[t] = sens_ref[t, 0].astype(jnp.float32)
    columns = [
        jnp.concatenate(
            [
                mixed[t, pl.ds(z * lines + line, devices, stride=group), :].astype(jnp.bfloat16)
                for t in range(2)
                for line in range(lines)
            ],
            axis=0,
        )
        for z in range(planes)
    ]
    done = dot(table_ref[...], jnp.concatenate(columns, axis=1))
    for z in range(planes):
        rr = done[:cells, z * width : (z + 1) * width]
        ri = done[cells:, z * width : (z + 1) * width]
        sr = wide[0, pl.ds(z, cells, stride=planes), :]
        si = wide[1, pl.ds(z, cells, stride=planes), :]
        total[0, z] += sr * rr + si * ri
        total[1, z] += sr * ri - si * rr

    @pl.when(coil == pl.num_programs(0) - 1)
    def _():
        out_ref[...] = total[...].astype(out_ref.dtype)


def removed(real, imaginary, limit):
    factor = jnp.minimum(lax.rsqrt(real * real + imaginary * imaginary) * limit, 1.0)
    return real * factor, imaginary * factor


def wavelet_kernel(planes, own_ref, low_ref, high_ref, limits_ref, out_ref, a0, lo0, hi0, a1, lo1, hi1, sums, diffs):
    rows, width = own_ref.shape[2], own_ref.shape[3]
    margin = low_ref.shape[1]
    count = planes + 2 * margin
    steps = rows // 8
    pad = 8
    for t in range(2):
        for p in range(margin):
            a0[t, p] = low_ref[t, p].astype(jnp.float32)
            a0[t, margin + planes + p] = high_ref[t, p].astype(jnp.float32)
        for p in range(planes):
            a0[t, margin + p] = own_ref[t, p]

    def split_lanes(source, lo, hi, lo_planes, hi_planes, offset):
        def step(j, carry):
            y = pl.multiple_of(j * 8, 8)
            for t in range(2):
                for p in lo_planes:
                    v = source[t, p, pl.ds(y, 8), :]
                    s = pltpu.roll(v, width - offset, 1)
                    lo[t, p, pl.ds(y, 8), :] = v + s
                    if p in hi_planes:
                        hi[t, p, pl.ds(y, 8), :] = v - s
            return carry

        lax.fori_loop(0, steps, step, 0)
        for t in range(2):
            for p in lo_planes:
                lo[t, p, rows : rows + 8] = lo[t, p, 0:8]
                if p in hi_planes:
                    hi[t, p, rows : rows + 8] = hi[t, p, 0:8]

    def detail_step(y, lo, hi, offset, level, first, last, coarse):
        for x_band, source in ((0, lo), (1, hi)):
            merged = []
            for y_band in range(2):
                band = x_band + 2 * y_band
                v = {}
                for p in range(first, last + offset + 1):
                    for t in range(2):
                        here = source[t, p, pl.ds(y, 8), :]
                        there = source[t, p, pl.ds(y + offset, 8), :]
                        v[p, t] = here + there if y_band == 0 else here - there
                plus, minus = {}, {}
                for p in range(first, last + 1):
                    high = removed(
                        v[p, 0] - v[p + offset, 0], v[p, 1] - v[p + offset, 1], limits_ref[level, band + 3]
                    )
                    if band:
                        low = removed(
                            v[p, 0] + v[p + offset, 0], v[p, 1] + v[p + offset, 1], limits_ref[level, band - 1]
                        )
                    elif coarse is not None:
                        low = (coarse[0, p, pl.ds(y, 8), :], coarse[1, p, pl.ds(y, 8), :])
                    else:
                        low = None
                    for t in range(2):
                        plus[p, t] = high[t] if low is None else low[t] + high[t]
                        minus[p, t] = -high[t] if low is None else low[t] - high[t]
                merged.append(
                    {
                        (p, t): plus[p, t] + minus[p - offset, t]
                        for p in range(first + offset, last + 1)
                        for t in range(2)
                    }
                )
            for p, t in merged[0]:
                sums[x_band, t, p, pl.ds(y, 8), :] = merged[0][p, t] + merged[1][p, t]
                diffs[x_band, t, p, pl.ds(y + pad, 8), :] = merged[0][p, t] - merged[1][p, t]

    def wrap_diffs(merged_planes):
        for x_band in range(2):
            for t in range(2):
                for p in merged_planes:
                    diffs[x_band, t, p, 0:pad] = diffs[x_band, t, p, rows : rows + pad]

    def merged_rows(y, t, p, offset):
        lower = sums[0, t, p, pl.ds(y, 8), :] + diffs[0, t, p, pl.ds(y + pad - offset, 8), :]
        upper = sums[1, t, p, pl.ds(y, 8), :] + diffs[1, t, p, pl.ds(y + pad - offset, 8), :]
        return lower + upper + pltpu.roll(lower - upper, offset, 1)

    split_lanes(a0, lo0, hi0, range(count), range(2, planes + 4), 1)

    def coarse_step(j, carry):
        y = pl.multiple_of(j * 8, 8)
        for t in range(2):
            v = [lo0[t, p, pl.ds(y, 8), :] + lo0[t, p, pl.ds(y + 1, 8), :] for p in range(count)]
            for p in range(count - 1):
                w = v[p] + v[p + 1]
                a1[t, p, pl.ds(y, 8), :] = w
        return carry

    lax.fori_loop(0, steps, coarse_step, 0)

    split_lanes(a1, lo1, hi1, range(count - 1), range(count - 1), 2)

    def level_one(j, carry):
        detail_step(pl.multiple_of(j * 8, 8), lo1, hi1, 2, 1, 0, planes + 2, None)
        return carry

    lax.fori_loop(0, steps, level_one, 0)
    wrap_diffs(range(2, planes + 3))

    def level_one_merge(j, carry):
        y = pl.multiple_of(j * 8, 8)
        for t in range(2):
            for p in range(2, planes + 3):
                a1[t, p, pl.ds(y, 8), :] = merged_rows(y, t, p, 2) * (1.0 / 64.0)
        return carry

    lax.fori_loop(0, steps, level_one_merge, 0)

    def level_zero(j, carry):
        detail_step(pl.multiple_of(j * 8, 8), lo0, hi0, 1, 0, 2, planes + 2, a1)
        return carry

    lax.fori_loop(0, steps, level_zero, 0)
    wrap_diffs(range(3, planes + 3))

    def level_zero_merge(j, carry):
        y = pl.multiple_of(j * 8, 8)
        for t in range(2):
            for p in range(planes):
                value = a0[t, margin + p, pl.ds(y, 8), :] - merged_rows(y, t, margin + p, 1) * (1.0 / 64.0)
                out_ref[t, pl.ds(y * planes + p, 8, stride=planes), :] = value
        return carry

    lax.fori_loop(0, steps, level_zero_merge, 0)


def whole(array):
    shape = array.shape
    return pl.BlockSpec(shape, lambda *_: (0,) * len(shape))


def shrink(own, low, high, thresholds):
    _, planes, rows, width = own.shape
    margin = low.shape[1]
    count = planes + 2 * margin
    scale = np.array([[2.0 ** (1.5 * (level + 1))] for level in range(thresholds.shape[0])], np.float32)
    limits = thresholds * scale
    f32 = jnp.float32
    buffers = [
        pltpu.VMEM((2, count, rows, width), f32),
        pltpu.VMEM((2, count, rows + 8, width), f32),
        pltpu.VMEM((2, count, rows + 8, width), f32),
        pltpu.VMEM((2, count, rows, width), f32),
        pltpu.VMEM((2, count, rows + 8, width), f32),
        pltpu.VMEM((2, count, rows + 8, width), f32),
        pltpu.VMEM((2, 2, count, rows, width), f32),
        pltpu.VMEM((2, 2, count, rows + 8, width), f32),
    ]

    def kernel(*refs):
        wavelet_kernel(planes, *refs)

    return pl.pallas_call(
        kernel,
        out_shape=jax.ShapeDtypeStruct((2, rows * planes, width), f32),
        in_specs=[
            pl.BlockSpec(memory_space=pltpu.VMEM),
            pl.BlockSpec(memory_space=pltpu.VMEM),
            pl.BlockSpec(memory_space=pltpu.VMEM),
            pl.BlockSpec(memory_space=pltpu.SMEM),
        ],
        out_specs=pl.BlockSpec(memory_space=pltpu.VMEM),
        scratch_shapes=buffers,
        name="wavelet",
    )(own, low, high, limits)


def local(image, sens, measured, mask, thresholds):
    _, phase_cells, planes, width = image.shape
    coils = sens.shape[1]
    lines, depth_cells = measured.shape[2], measured.shape[3]
    devices = lax.axis_size(lines_axes)
    group = lines * planes
    per_chunk = coils // chunk_count
    bf16, f32 = jnp.bfloat16, jnp.float32

    order = (np.arange(devices)[None, :] * lines + np.arange(lines)[:, None]).reshape(-1)
    table_phase = fourier_table(phase_cells, -1.0, rows=order)
    inverse_phase = fourier_table(phase_cells, 1.0, columns=order)
    table_depth = fourier_table(depth_cells, -1.0)
    inverse_depth = fourier_table(depth_cells, 1.0)
    inverse_readout = fourier_table(width, 1.0).T.reshape(2, width, 2, width)

    image_rows = image.reshape(2, phase_cells * planes, width)
    sens_rows = sens.reshape(2, coils, phase_cells * planes, width)
    block = (devices, 2, 1, group, width)
    exchanged = jax.ShapeDtypeStruct((devices, 2, per_chunk, group, width), bf16)
    exchanged_spec = pl.BlockSpec(block, lambda c: (0, 0, c, 0, 0))
    plane_shape = (2, planes, phase_cells, width)

    def forward(chunk):
        def kernel(*refs):
            forward_kernel(devices, lines, planes, *refs)

        return pl.pallas_call(
            kernel,
            grid=(per_chunk,),
            out_shape=exchanged,
            in_specs=[
                pl.BlockSpec((2, 1, phase_cells * planes, width), lambda c: (0, c + chunk * per_chunk, 0, 0)),
                whole(image_rows),
                whole(table_phase),
            ],
            out_specs=exchanged_spec,
            scratch_shapes=[pltpu.VMEM((2, phase_cells * planes, width), f32)] * 2,
            name="forward",
        )(sens_rows, image_rows, table_phase)

    def middle(received, own_measured, wide_mask, chunk):
        def kernel(*refs):
            middle_kernel(lines, *refs)

        return pl.pallas_call(
            kernel,
            grid=(per_chunk,),
            out_shape=exchanged,
            in_specs=[
                exchanged_spec,
                pl.BlockSpec((2, 1, lines, depth_cells, width), lambda c: (0, c + chunk * per_chunk, 0, 0, 0)),
                whole(wide_mask),
                whole(table_depth),
                whole(inverse_depth),
            ],
            out_specs=exchanged_spec,
            scratch_shapes=[pltpu.VMEM((2, depth_cells * lines, width), f32)] * 2,
            name="middle",
        )(received, own_measured, wide_mask, table_depth, inverse_depth)

    def backward(received, chunk, first):
        specs = [
            exchanged_spec,
            pl.BlockSpec((2, 1, phase_cells * planes, width), lambda c: (0, c + chunk * per_chunk, 0, 0)),
            whole(inverse_phase),
        ]
        operands = [received, sens_rows, inverse_phase]
        if first is None:

            def kernel(*refs):
                backward_kernel(lines, planes, None, *refs)

        else:
            specs.insert(0, whole(first))
            operands.insert(0, first)

            def kernel(*refs):
                backward_kernel(lines, planes, *refs)

        return pl.pallas_call(
            kernel,
            grid=(per_chunk,),
            out_shape=jax.ShapeDtypeStruct(plane_shape, bf16 if chunk == chunk_count - 1 else f32),
            in_specs=specs,
            out_specs=pl.BlockSpec(plane_shape, lambda c: (0, 0, 0, 0)),
            scratch_shapes=[pltpu.VMEM((2, phase_cells * planes, width), f32)] * 2
            + [pltpu.VMEM(plane_shape, f32)],
            name="backward",
        )(*operands)

    def exchange(values):
        return lax.all_to_all(values, lines_axes, 0, 0, tiled=True)

    received = [exchange(forward(chunk)) for chunk in range(chunk_count)]
    own_measured = jnp.einsum(
        "tclzk,tksx->sclzx", measured, inverse_readout, preferred_element_type=f32
    ).astype(bf16)
    wide_mask = jnp.broadcast_to(mask.astype(f32)[:, :, None], (lines, depth_cells, width))
    image_planes = jnp.transpose(image, (0, 2, 1, 3))
    returned = [
        exchange(middle(received[chunk], own_measured, wide_mask, chunk)) for chunk in range(chunk_count)
    ]
    total = None
    for chunk in range(chunk_count):
        total = backward(returned[chunk], chunk, total)

    size = lax.axis_size("coil")
    copies = lax.all_to_all(jnp.broadcast_to(total[None], (size, *total.shape)), "coil", 0, 0, tiled=True)
    gradient = copies.astype(f32).sum(axis=0)
    own = image_planes - step_size * gradient
    margin = 2 ** thresholds.shape[0] - 1
    up = [(i, (i + 1) % devices) for i in range(devices)]
    down = [(target, source) for source, target in up]
    narrow = own.astype(bf16)
    low = lax.ppermute(narrow[:, planes - margin :], lines_axes, up)
    high = lax.ppermute(narrow[:, :margin], lines_axes, down)
    result = shrink(own, low, high, thresholds)
    return result.reshape(2, phase_cells, planes, width)


def solution(mesh):
    return jax.shard_map(
        local,
        mesh=mesh,
        in_specs=(
            P("groups", None, lines_axes, None),
            P("groups", "coil", None, lines_axes, None),
            P("groups", "coil", lines_axes, None, None),
            P(lines_axes, None),
            P(),
        ),
        out_specs=P("groups", None, lines_axes, None),
        check_vma=False,
    )
```

```python
import math

import jax
import jax.numpy as jnp
import ml_dtypes
import numpy as np
from jax import lax
from jax.experimental import pallas as pl
from jax.experimental.pallas import tpu as pltpu
from jax.sharding import PartitionSpec as P

step_size = 0.5
lines_axes = ("slab", "row")
pause_steps = 6500


def fourier_table(length, sign, rows=None, columns=None):
    index = np.arange(length, dtype=np.int64)
    phase = (index[:, None] * index[None, :]) % length
    theta = phase.astype(np.float32) * np.float32(2.0 * math.pi / length)
    scale = np.float32(1.0 / math.sqrt(length))
    real = (np.cos(theta) * scale).astype(np.float32)
    imaginary = (np.sin(theta) * np.float32(sign) * scale).astype(np.float32)
    if rows is not None:
        real, imaginary = real[rows], imaginary[rows]
    if columns is not None:
        real, imaginary = real[:, columns], imaginary[:, columns]
    return np.block([[real, -imaginary], [imaginary, real]]).astype(ml_dtypes.bfloat16)


def dot(left, right):
    return jnp.dot(left, right, preferred_element_type=jnp.float32)


def forward_kernel(slabs, lines, planes, sens_ref, image_ref, table_ref, out_ref, product, mixed):
    cells = product.shape[1] // planes
    group = lines * planes
    sr = sens_ref[0, 0].astype(jnp.float32)
    si = sens_ref[1, 0].astype(jnp.float32)
    ir = image_ref[0]
    ii = image_ref[1]
    product[0] = sr * ir - si * ii
    product[1] = sr * ii + si * ir
    columns = [
        jnp.concatenate(
            [product[t, pl.ds(z, cells, stride=planes), :].astype(jnp.bfloat16) for t in range(2)],
            axis=0,
        )
        for z in range(planes)
    ]
    done = dot(table_ref[...], jnp.concatenate(columns, axis=1))
    width = product.shape[2]
    for s in range(2):
        for z in range(planes):
            for line in range(lines):
                first = s * cells + line * slabs
                mixed[s, pl.ds(z * lines + line, slabs, stride=group), :] = done[
                    first : first + slabs, z * width : (z + 1) * width
                ]
        out_ref[:, s, 0] = mixed[s].astype(jnp.bfloat16).reshape(slabs, group, width)


def middle_kernel(lines, lower_ref, upper_ref, measured_ref, mask_ref, table_ref, inverse_ref, out_ref, mixed, back):
    slabs, _, _, _, group, width = lower_ref.shape
    half = slabs * group // lines
    cells = 2 * half
    for row, ref in enumerate((lower_ref, upper_ref)):
        for t in range(2):
            mixed[row, t] = ref[:, 0, t, 0].astype(jnp.float32).reshape(slabs * group, width)
    columns = [
        jnp.concatenate(
            [
                mixed[row, t, pl.ds(line, half, stride=lines), :].astype(jnp.bfloat16)
                for t in range(2)
                for row in range(2)
            ],
            axis=0,
        )
        for line in range(lines)
    ]
    spectrum = dot(table_ref[...], jnp.concatenate(columns, axis=1))
    residual = []
    for line in range(lines):
        parts = []
        for t in range(2):
            value = spectrum[t * cells : (t + 1) * cells, line * width : (line + 1) * width]
            value = mask_ref[line] * (value - measured_ref[t, 0, line].astype(jnp.float32))
            parts.append(value.astype(jnp.bfloat16))
        residual.append(jnp.concatenate(parts, axis=0))
    result = dot(inverse_ref[...], jnp.concatenate(residual, axis=1))
    for row in range(2):
        for s in range(2):
            first = s * cells + row * half
            for line in range(lines):
                back[row, s, pl.ds(line, half, stride=lines), :] = result[
                    first : first + half, line * width : (line + 1) * width
                ]
            out_ref[:, row, s, 0] = back[row, s].astype(jnp.bfloat16).reshape(slabs, group, width)


def backward_kernel(lines, planes, edge, in_ref, sens_ref, table_ref, out_ref, mixed, wide, total, framed):
    slabs, rows, _, _, group, width = in_ref.shape
    cells = slabs * lines
    coil = pl.program_id(0)

    @pl.when(coil == 0)
    def _():
        total[...] = jnp.zeros(total.shape, jnp.float32)

    for row in range(rows):
        for t in range(2):
            mixed[row, t] = in_ref[:, row, t, 0].astype(jnp.float32).reshape(slabs * group, width)
            wide[row, t] = sens_ref[t, 0, row].astype(jnp.float32)
    columns = [
        jnp.concatenate(
            [
                mixed[row, t, pl.ds(z * lines + line, slabs, stride=group), :].astype(jnp.bfloat16)
                for t in range(2)
                for line in range(lines)
            ],
            axis=0,
        )
        for row in range(rows)
        for z in range(planes)
    ]
    done = dot(table_ref[...], jnp.concatenate(columns, axis=1))
    for row in range(rows):
        for z in range(planes):
            plane = row * planes + z
            rr = done[:cells, plane * width : (plane + 1) * width]
            ri = done[cells:, plane * width : (plane + 1) * width]
            sr = wide[row, 0, pl.ds(z, cells, stride=planes), :]
            si = wide[row, 1, pl.ds(z, cells, stride=planes), :]
            total[row, 0, z] += sr * rr + si * ri
            total[row, 1, z] += sr * ri - si * rr

    @pl.when(coil == pl.num_programs(0) - 1)
    def _():
        pieces, _, _, tall, _ = out_ref.shape
        step = tall - 2 * edge
        for row in range(rows):
            for t in range(2):
                for z in range(planes):
                    framed[0:edge] = total[row, t, z, cells - edge : cells]
                    framed[edge : edge + cells] = total[row, t, z]
                    framed[edge + cells :] = total[row, t, z, 0:edge]
                    for q in range(pieces // rows):
                        out_ref[q * rows + row, t, z] = framed[q * step : q * step + tall].astype(out_ref.dtype)


def removed(real, imaginary, limit):
    factor = jnp.minimum(lax.rsqrt(real * real + imaginary * imaginary) * limit, 1.0)
    return real * factor, imaginary * factor


def wavelet_kernel(edge, image_ref, own_ref, low_ref, high_ref, limits_ref, out_ref, a0, lo0, hi0, a1, lo1, hi1, sums, diffs, mixed):
    planes, rows, width = own_ref.shape[1:]
    margin = low_ref.shape[1]
    count = planes + 2 * margin
    steps = rows // 8
    pad = 8
    for t in range(2):
        for p in range(margin):
            a0[t, p] = low_ref[t, p].astype(jnp.float32)
            a0[t, margin + planes + p] = high_ref[t, p].astype(jnp.float32)
        for p in range(planes):
            a0[t, margin + p] = own_ref[t, p]

    def split_lanes(source, lo, hi, lo_planes, hi_planes, offset):
        def step(j, carry):
            y = pl.multiple_of(j * 8, 8)
            for t in range(2):
                for p in lo_planes:
                    v = source[t, p, pl.ds(y, 8), :]
                    s = pltpu.roll(v, width - offset, 1)
                    lo[t, p, pl.ds(y, 8), :] = v + s
                    if p in hi_planes:
                        hi[t, p, pl.ds(y, 8), :] = v - s
            return carry

        lax.fori_loop(0, steps, step, 0)

    def detail_step(y, lo, hi, offset, level, first, last, coarse):
        for x_band, source in ((0, lo), (1, hi)):
            merged = []
            for y_band in range(2):
                band = x_band + 2 * y_band
                v = {}
                for p in range(first, last + offset + 1):
                    for t in range(2):
                        here = source[t, p, pl.ds(y, 8), :]
                        there = source[t, p, pl.ds(y + offset, 8), :]
                        v[p, t] = here + there if y_band == 0 else here - there
                plus, minus = {}, {}
                for p in range(first, last + 1):
                    high = removed(
                        v[p, 0] - v[p + offset, 0], v[p, 1] - v[p + offset, 1], limits_ref[level, band + 3]
                    )
                    if band:
                        low = removed(
                            v[p, 0] + v[p + offset, 0], v[p, 1] + v[p + offset, 1], limits_ref[level, band - 1]
                        )
                    elif coarse is not None:
                        low = (coarse[0, p, pl.ds(y, 8), :], coarse[1, p, pl.ds(y, 8), :])
                    else:
                        low = None
                    for t in range(2):
                        plus[p, t] = high[t] if low is None else low[t] + high[t]
                        minus[p, t] = -high[t] if low is None else low[t] - high[t]
                merged.append(
                    {
                        (p, t): plus[p, t] + minus[p - offset, t]
                        for p in range(first + offset, last + 1)
                        for t in range(2)
                    }
                )
            for p, t in merged[0]:
                sums[x_band, t, p, pl.ds(y, 8), :] = merged[0][p, t] + merged[1][p, t]
                diffs[x_band, t, p, pl.ds(y + pad, 8), :] = merged[0][p, t] - merged[1][p, t]

    def merged_rows(y, t, p, offset):
        lower = sums[0, t, p, pl.ds(y, 8), :] + diffs[0, t, p, pl.ds(y + pad - offset, 8), :]
        upper = sums[1, t, p, pl.ds(y, 8), :] + diffs[1, t, p, pl.ds(y + pad - offset, 8), :]
        return lower + upper + pltpu.roll(lower - upper, offset, 1)

    split_lanes(a0, lo0, hi0, range(count), range(2, planes + 4), 1)

    def coarse_step(j, carry):
        y = pl.multiple_of(j * 8, 8)
        for t in range(2):
            v = [lo0[t, p, pl.ds(y, 8), :] + lo0[t, p, pl.ds(y + 1, 8), :] for p in range(count)]
            for p in range(count - 1):
                w = v[p] + v[p + 1]
                a1[t, p, pl.ds(y, 8), :] = w
        return carry

    lax.fori_loop(0, steps, coarse_step, 0)

    split_lanes(a1, lo1, hi1, range(count - 1), range(count - 1), 2)

    def level_one(j, carry):
        detail_step(pl.multiple_of(j * 8, 8), lo1, hi1, 2, 1, 0, planes + 2, None)
        return carry

    lax.fori_loop(0, steps, level_one, 0)

    def level_one_merge(j, carry):
        y = pl.multiple_of(j * 8, 8)
        for t in range(2):
            for p in range(2, planes + 3):
                a1[t, p, pl.ds(y, 8), :] = merged_rows(y, t, p, 2) * (1.0 / 64.0)
        return carry

    lax.fori_loop(0, steps, level_one_merge, 0)

    def level_zero(j, carry):
        detail_step(pl.multiple_of(j * 8, 8), lo0, hi0, 1, 0, 2, planes + 2, a1)
        return carry

    lax.fori_loop(0, steps, level_zero, 0)

    def level_zero_merge(j, carry):
        y = pl.multiple_of(j * 8, 8)
        for t in range(2):
            for p in range(planes):
                change = own_ref[t, p, pl.ds(y, 8), :] - image_ref[t, p, pl.ds(y, 8), :]
                change = change - merged_rows(y, t, margin + p, 1) * (1.0 / 64.0)
                mixed[t, pl.ds(y * planes + p, 8, stride=planes), :] = change
        return carry

    lax.fori_loop(0, steps, level_zero_merge, 0)
    for t in range(2):
        kept = mixed[t, edge * planes : (rows - edge) * planes].astype(out_ref.dtype)
        for copy in range(out_ref.shape[0]):
            out_ref[copy, t] = kept


def whole(array):
    shape = array.shape
    return pl.BlockSpec(shape, lambda *_: (0,) * len(shape))


def shrink(image, own, low, high, thresholds, edge, copies):
    _, planes, rows, width = own.shape
    margin = low.shape[1]
    count = planes + 2 * margin
    scale = np.array([[2.0 ** (1.5 * (level + 1))] for level in range(thresholds.shape[0])], np.float32)
    limits = thresholds * scale
    f32 = jnp.float32
    buffers = [
        pltpu.VMEM((2, count, rows, width), f32),
        pltpu.VMEM((2, count, rows + 8, width), f32),
        pltpu.VMEM((2, count, rows + 8, width), f32),
        pltpu.VMEM((2, count, rows, width), f32),
        pltpu.VMEM((2, count, rows + 8, width), f32),
        pltpu.VMEM((2, count, rows + 8, width), f32),
        pltpu.VMEM((2, 2, count, rows, width), f32),
        pltpu.VMEM((2, 2, count, rows + 8, width), f32),
        pltpu.VMEM((2, rows * planes, width), f32),
    ]

    def kernel(*refs):
        wavelet_kernel(edge, *refs)

    return pl.pallas_call(
        kernel,
        out_shape=jax.ShapeDtypeStruct((copies, 2, (rows - 2 * edge) * planes, width), jnp.bfloat16),
        in_specs=[pl.BlockSpec(memory_space=pltpu.VMEM)] * 4 + [pl.BlockSpec(memory_space=pltpu.SMEM)],
        out_specs=pl.BlockSpec(memory_space=pltpu.VMEM),
        scratch_shapes=buffers,
        name="wavelet",
    )(image, own, low, high, limits)


def local(image, sens, measured, mask, thresholds):
    _, phase_cells, planes, width = image.shape
    coils = sens.shape[1]
    own_lines, depth_cells = measured.shape[2], measured.shape[3]
    slabs, rows, columns = (lax.axis_size(name) for name in ("slab", "row", "coil"))
    row = lax.axis_index("row")
    lines = own_lines * rows
    group = lines * planes
    half = coils // rows
    bf16, f32 = jnp.bfloat16, jnp.float32
    other = [(0, 1), (1, 0)]

    order = (np.arange(slabs)[None, :] * lines + np.arange(lines)[:, None]).reshape(-1)
    depth_order = np.arange(depth_cells).reshape(slabs, rows, planes).transpose(1, 0, 2).reshape(-1)
    table_phase = fourier_table(phase_cells, -1.0, rows=order)
    inverse_phase = fourier_table(phase_cells, 1.0, columns=order)
    table_depth = fourier_table(depth_cells, -1.0, columns=depth_order)
    inverse_depth = fourier_table(depth_cells, 1.0, rows=depth_order)
    inverse_readout = fourier_table(width, 1.0).T.reshape(2, width, 2, width)

    image_rows = image.reshape(2, phase_cells * planes, width)
    sens_rows = sens.reshape(2, coils, phase_cells * planes, width)
    sens_spec = (2, 1, phase_cells * planes, width)
    piece = (slabs, 2, half, group, width)
    exchanged = jax.ShapeDtypeStruct((slabs, rows, 2, half, group, width), bf16)
    stack = pltpu.VMEM((2, phase_cells * planes, width), f32)
    here = row.astype(jnp.int32).reshape(1)

    def given(kernel, grid_spec, out_shape, name):
        return pl.pallas_call(kernel, grid_spec=grid_spec, out_shape=out_shape, name=name)

    def send_kernel(_, *refs):
        forward_kernel(slabs, lines, planes, *refs)

    sent = given(
        send_kernel,
        pltpu.PrefetchScalarGridSpec(
            num_scalar_prefetch=1,
            grid=(half,),
            in_specs=[
                pl.BlockSpec(sens_spec, lambda c, r: (0, (1 - r[0]) * half + c, 0, 0)),
                whole(image_rows),
                whole(table_phase),
            ],
            out_specs=pl.BlockSpec((slabs, 2, 1, group, width), lambda c, r: (0, 0, c, 0, 0)),
            scratch_shapes=[stack, stack],
        ),
        jax.ShapeDtypeStruct(piece, bf16),
        "forward_sent",
    )(here, sens_rows, image_rows, table_phase)
    arrived = lax.ppermute(sent, "row", other)

    def keep_kernel(r_ref, sens_ref, image_ref, table_ref, arrived_ref, out_ref, pause_ref, product, mixed):
        @pl.when(pl.program_id(0) == 0)
        def _():
            pause_ref[...] = lax.fori_loop(
                0, r_ref[0] * pause_steps, lambda _, v: v * 1.0001 + 0.5, jnp.ones(pause_ref.shape, jnp.float32)
            )

        forward_kernel(slabs, lines, planes, sens_ref, image_ref, table_ref, out_ref.at[:, 0], product, mixed)
        out_ref[:, 1] = arrived_ref[...]

    outgoing, _ = given(
        keep_kernel,
        pltpu.PrefetchScalarGridSpec(
            num_scalar_prefetch=1,
            grid=(half,),
            in_specs=[
                pl.BlockSpec(sens_spec, lambda c, r: (0, r[0] * half + c, 0, 0)),
                whole(image_rows),
                whole(table_phase),
                pl.BlockSpec((slabs, 2, 1, group, width), lambda c, r: (0, 0, c, 0, 0)),
            ],
            out_specs=[
                pl.BlockSpec((slabs, rows, 2, 1, group, width), lambda c, r: (0, 0, 0, c, 0, 0)),
                pl.BlockSpec((8, 128), lambda c, r: (0, 0)),
            ],
            scratch_shapes=[stack, stack],
        ),
        [exchanged, jax.ShapeDtypeStruct((8, 128), f32)],
        "forward_kept",
    )(here, sens_rows, image_rows, table_phase, arrived)

    received = lax.all_to_all(outgoing, "slab", 0, 0, tiled=True)

    measured, mask, sens_late, image, _ = lax.optimization_barrier((measured, mask, sens_rows, image, outgoing))

    def both_rows(values, axis):
        kept = lax.dynamic_slice_in_dim(values, row * half, half, axis=1)
        away = lax.dynamic_slice_in_dim(values, (1 - row) * half, half, axis=1)
        return in_row_order(kept, lax.ppermute(away, "row", other), axis)

    def in_row_order(own, others, axis):
        first = row == 0
        return jnp.concatenate([jnp.where(first, own, others), jnp.where(first, others, own)], axis=axis)

    own_measured = jnp.einsum(
        "tclzk,tksx->sclzx", measured, inverse_readout, preferred_element_type=f32
    ).astype(bf16)
    chip_measured = both_rows(own_measured, 2)
    own_mask = mask.astype(f32)
    chip_mask = in_row_order(own_mask, lax.ppermute(own_mask, "row", other), 0)
    wide_mask = jnp.broadcast_to(chip_mask[:, :, None], (lines, depth_cells, width))
    chip_sens = both_rows(sens_late[:, :, None], 2)
    edge = 4
    quarter = phase_cells // columns
    image_planes = jnp.transpose(image, (0, 2, 1, 3))
    framed = jnp.concatenate(
        [image_planes[:, :, phase_cells - edge :], image_planes, image_planes[:, :, :edge]], axis=2
    )
    own_image = lax.dynamic_slice_in_dim(
        framed, lax.axis_index("coil") * quarter, quarter + 2 * edge, axis=2
    )

    def mid_kernel(_, *refs):
        middle_kernel(lines, *refs)

    block = (slabs, 1, 2, 1, group, width)
    buffer = pltpu.VMEM((rows, 2, slabs * group, width), f32)
    returning = given(
        mid_kernel,
        pltpu.PrefetchScalarGridSpec(
            num_scalar_prefetch=1,
            grid=(half,),
            in_specs=[
                pl.BlockSpec(block, lambda c, r: (0, r[0], 0, c, 0, 0)),
                pl.BlockSpec(block, lambda c, r: (0, 1 - r[0], 0, c, 0, 0)),
                pl.BlockSpec((2, 1, lines, depth_cells, width), lambda c, r: (0, c, 0, 0, 0)),
                whole(wide_mask),
                whole(table_depth),
                whole(inverse_depth),
            ],
            out_specs=pl.BlockSpec((slabs, rows, 2, 1, group, width), lambda c, r: (0, 0, 0, c, 0, 0)),
            scratch_shapes=[buffer, buffer],
        ),
        exchanged,
        "middle",
    )(here, received, received, chip_measured, wide_mask, table_depth, inverse_depth)
    returned = lax.all_to_all(returning, "slab", 0, 0, tiled=True)

    tall = quarter + 2 * edge

    def back_kernel(*refs):
        backward_kernel(lines, planes, edge, *refs)

    parts = pl.pallas_call(
        back_kernel,
        grid=(half,),
        out_shape=jax.ShapeDtypeStruct((columns * rows, 2, planes, tall, width), bf16),
        in_specs=[
            pl.BlockSpec((slabs, rows, 2, 1, group, width), lambda c: (0, 0, 0, c, 0, 0)),
            pl.BlockSpec((2, 1, rows, phase_cells * planes, width), lambda c: (0, c, 0, 0, 0)),
            whole(inverse_phase),
        ],
        out_specs=pl.BlockSpec((columns * rows, 2, planes, tall, width), lambda c: (0, 0, 0, 0, 0)),
        scratch_shapes=[
            buffer,
            buffer,
            pltpu.VMEM((rows, 2, planes, phase_cells, width), f32),
            pltpu.VMEM((phase_cells + 2 * edge, width), f32),
        ],
        name="backward",
    )(returned, chip_sens, inverse_phase)
    gradient = lax.all_to_all(parts, ("coil", "row"), 0, 0, tiled=True).astype(f32).sum(axis=0)
    own = own_image - step_size * gradient
    margin = 2 ** thresholds.shape[0] - 1
    devices = slabs * rows
    up = [(i, (i + 1) % devices) for i in range(devices)]
    down = [(target, source) for source, target in up]
    narrow = own.astype(bf16)
    low = lax.ppermute(narrow[:, planes - margin :], lines_axes, up)
    high = lax.ppermute(narrow[:, :margin], lines_axes, down)
    change = shrink(own_image, own, low, high, thresholds, edge, columns)
    gathered = lax.all_to_all(change, "coil", 0, 0, tiled=True)
    change_rows = jnp.swapaxes(gathered, 0, 1).reshape(2, phase_cells * planes, width)
    return (image_rows + change_rows.astype(f32)).reshape(2, phase_cells, planes, width)


def solution(mesh):
    return jax.shard_map(
        local,
        mesh=mesh,
        in_specs=(
            P("groups", None, lines_axes, None),
            P("groups", "coil", None, lines_axes, None),
            P("groups", "coil", lines_axes, None, None),
            P(lines_axes, None),
            P(),
        ),
        out_specs=P("groups", None, lines_axes, None),
        check_vma=False,
    )
```

```python
import math

import jax
import jax.numpy as jnp
import ml_dtypes
import numpy as np
from jax import lax
from jax.experimental import pallas as pl
from jax.experimental.pallas import tpu as pltpu
from jax.sharding import PartitionSpec as P

step_size = 0.5
lines_axes = ("slab", "row")
pause_steps = 6500


def fourier_table(length, sign, rows=None, columns=None):
    index = np.arange(length, dtype=np.int64)
    phase = (index[:, None] * index[None, :]) % length
    theta = phase.astype(np.float32) * np.float32(2.0 * math.pi / length)
    scale = np.float32(1.0 / math.sqrt(length))
    real = (np.cos(theta) * scale).astype(np.float32)
    imaginary = (np.sin(theta) * np.float32(sign) * scale).astype(np.float32)
    if rows is not None:
        real, imaginary = real[rows], imaginary[rows]
    if columns is not None:
        real, imaginary = real[:, columns], imaginary[:, columns]
    return np.block([[real, -imaginary], [imaginary, real]]).astype(ml_dtypes.bfloat16)


def dot(left, right):
    return jnp.dot(left, right, preferred_element_type=jnp.float32)


def forward_kernel(slabs, lines, planes, sens_ref, image_ref, table_ref, out_ref, product, mixed):
    cells = product.shape[1] // planes
    group = lines * planes
    sr = sens_ref[0, 0].astype(jnp.float32)
    si = sens_ref[1, 0].astype(jnp.float32)
    ir = image_ref[0]
    ii = image_ref[1]
    product[0] = sr * ir - si * ii
    product[1] = sr * ii + si * ir
    columns = [
        jnp.concatenate(
            [product[t, pl.ds(z, cells, stride=planes), :].astype(jnp.bfloat16) for t in range(2)],
            axis=0,
        )
        for z in range(planes)
    ]
    done = dot(table_ref[...], jnp.concatenate(columns, axis=1))
    width = product.shape[2]
    for s in range(2):
        for z in range(planes):
            for line in range(lines):
                first = s * cells + line * slabs
                mixed[s, pl.ds(z * lines + line, slabs, stride=group), :] = done[
                    first : first + slabs, z * width : (z + 1) * width
                ]
        out_ref[:, s, 0] = mixed[s].astype(jnp.bfloat16).reshape(slabs, group, width)


def middle_kernel(lines, lower_ref, upper_ref, measured_ref, mask_ref, table_ref, inverse_ref, out_ref, mixed, back):
    slabs, _, _, _, group, width = lower_ref.shape
    half = slabs * group // lines
    cells = 2 * half
    for row, ref in enumerate((lower_ref, upper_ref)):
        for t in range(2):
            mixed[row, t] = ref[:, 0, t, 0].astype(jnp.float32).reshape(slabs * group, width)
    columns = [
        jnp.concatenate(
            [
                mixed[row, t, pl.ds(line, half, stride=lines), :].astype(jnp.bfloat16)
                for t in range(2)
                for row in range(2)
            ],
            axis=0,
        )
        for line in range(lines)
    ]
    spectrum = dot(table_ref[...], jnp.concatenate(columns, axis=1))
    residual = []
    for line in range(lines):
        parts = []
        for t in range(2):
            value = spectrum[t * cells : (t + 1) * cells, line * width : (line + 1) * width]
            value = mask_ref[line] * (value - measured_ref[t, 0, line].astype(jnp.float32))
            parts.append(value.astype(jnp.bfloat16))
        residual.append(jnp.concatenate(parts, axis=0))
    result = dot(inverse_ref[...], jnp.concatenate(residual, axis=1))
    for row in range(2):
        for s in range(2):
            first = s * cells + row * half
            for line in range(lines):
                back[row, s, pl.ds(line, half, stride=lines), :] = result[
                    first : first + half, line * width : (line + 1) * width
                ]
            out_ref[:, row, s, 0] = back[row, s].astype(jnp.bfloat16).reshape(slabs, group, width)


def backward_kernel(lines, planes, edge, in_ref, sens_ref, table_ref, out_ref, mixed, wide, total, framed):
    slabs, rows, _, _, group, width = in_ref.shape
    cells = slabs * lines
    coil = pl.program_id(0)

    @pl.when(coil == 0)
    def _():
        total[...] = jnp.zeros(total.shape, jnp.float32)

    for row in range(rows):
        for t in range(2):
            mixed[row, t] = in_ref[:, row, t, 0].astype(jnp.float32).reshape(slabs * group, width)
            wide[row, t] = sens_ref[t, 0, row].astype(jnp.float32)
    columns = [
        jnp.concatenate(
            [
                mixed[row, t, pl.ds(z * lines + line, slabs, stride=group), :].astype(jnp.bfloat16)
                for t in range(2)
                for line in range(lines)
            ],
            axis=0,
        )
        for row in range(rows)
        for z in range(planes)
    ]
    done = dot(table_ref[...], jnp.concatenate(columns, axis=1))
    for row in range(rows):
        for z in range(planes):
            plane = row * planes + z
            rr = done[:cells, plane * width : (plane + 1) * width]
            ri = done[cells:, plane * width : (plane + 1) * width]
            sr = wide[row, 0, pl.ds(z, cells, stride=planes), :]
            si = wide[row, 1, pl.ds(z, cells, stride=planes), :]
            total[row, 0, z] += sr * rr + si * ri
            total[row, 1, z] += sr * ri - si * rr

    @pl.when(coil == pl.num_programs(0) - 1)
    def _():
        pieces, _, _, tall, _ = out_ref.shape
        step = tall - 2 * edge
        for row in range(rows):
            for t in range(2):
                for z in range(planes):
                    framed[0:edge] = total[row, t, z, cells - edge : cells]
                    framed[edge : edge + cells] = total[row, t, z]
                    framed[edge + cells :] = total[row, t, z, 0:edge]
                    for q in range(pieces):
                        out_ref[q, t, row * planes + z] = framed[q * step : q * step + tall].astype(out_ref.dtype)


def removed(real, imaginary, limit):
    factor = jnp.minimum(lax.rsqrt(real * real + imaginary * imaginary) * limit, 1.0)
    return real * factor, imaginary * factor


def wavelet_kernel(edge, margin, row_ref, chip_ref, halo_ref, limits_ref, out_ref, a0, lo0, hi0, a1, lo1, hi1, sums, diffs, mixed):
    chip_planes, rows, width = chip_ref.shape[1:]
    planes = chip_planes // 2
    count = planes + 2 * margin
    steps = rows // 8
    pad = 8
    row = row_ref[0]
    for t in range(2):
        for p in range(chip_planes):
            a0[t, (1 - row) * planes + p] = chip_ref[t, p]
        for p in range(margin):
            a0[t, 1 + row * (margin + planes) + p] = halo_ref[t, p].astype(jnp.float32)

    def split_lanes(source, shift, lo, hi, lo_planes, hi_planes, offset):
        def step(j, carry):
            y = pl.multiple_of(j * 8, 8)
            for t in range(2):
                for p in lo_planes:
                    v = source[t, p + shift, pl.ds(y, 8), :]
                    s = pltpu.roll(v, width - offset, 1)
                    lo[t, p, pl.ds(y, 8), :] = v + s
                    if p in hi_planes:
                        hi[t, p, pl.ds(y, 8), :] = v - s
            return carry

        lax.fori_loop(0, steps, step, 0)

    def detail_step(y, lo, hi, offset, level, first, last, coarse):
        for x_band, source in ((0, lo), (1, hi)):
            merged = []
            for y_band in range(2):
                band = x_band + 2 * y_band
                v = {}
                for p in range(first, last + offset + 1):
                    for t in range(2):
                        here = source[t, p, pl.ds(y, 8), :]
                        there = source[t, p, pl.ds(y + offset, 8), :]
                        v[p, t] = here + there if y_band == 0 else here - there
                plus, minus = {}, {}
                for p in range(first, last + 1):
                    high = removed(
                        v[p, 0] - v[p + offset, 0], v[p, 1] - v[p + offset, 1], limits_ref[level, band + 3]
                    )
                    if band:
                        low = removed(
                            v[p, 0] + v[p + offset, 0], v[p, 1] + v[p + offset, 1], limits_ref[level, band - 1]
                        )
                    elif coarse is not None:
                        low = (coarse[0, p, pl.ds(y, 8), :], coarse[1, p, pl.ds(y, 8), :])
                    else:
                        low = None
                    for t in range(2):
                        plus[p, t] = high[t] if low is None else low[t] + high[t]
                        minus[p, t] = -high[t] if low is None else low[t] - high[t]
                merged.append(
                    {
                        (p, t): plus[p, t] + minus[p - offset, t]
                        for p in range(first + offset, last + 1)
                        for t in range(2)
                    }
                )
            for p, t in merged[0]:
                sums[x_band, t, p, pl.ds(y, 8), :] = merged[0][p, t] + merged[1][p, t]
                diffs[x_band, t, p, pl.ds(y + pad, 8), :] = merged[0][p, t] - merged[1][p, t]

    def merged_rows(y, t, p, offset):
        lower = sums[0, t, p, pl.ds(y, 8), :] + diffs[0, t, p, pl.ds(y + pad - offset, 8), :]
        upper = sums[1, t, p, pl.ds(y, 8), :] + diffs[1, t, p, pl.ds(y + pad - offset, 8), :]
        return lower + upper + pltpu.roll(lower - upper, offset, 1)

    split_lanes(a0, 1, lo0, hi0, range(count), range(2, planes + 4), 1)

    def coarse_step(j, carry):
        y = pl.multiple_of(j * 8, 8)
        for t in range(2):
            v = [lo0[t, p, pl.ds(y, 8), :] + lo0[t, p, pl.ds(y + 1, 8), :] for p in range(count)]
            for p in range(count - 1):
                w = v[p] + v[p + 1]
                a1[t, p, pl.ds(y, 8), :] = w
        return carry

    lax.fori_loop(0, steps, coarse_step, 0)

    split_lanes(a1, 0, lo1, hi1, range(count - 1), range(count - 1), 2)

    def level_one(j, carry):
        detail_step(pl.multiple_of(j * 8, 8), lo1, hi1, 2, 1, 0, planes + 2, None)
        return carry

    lax.fori_loop(0, steps, level_one, 0)

    def level_one_merge(j, carry):
        y = pl.multiple_of(j * 8, 8)
        for t in range(2):
            for p in range(2, planes + 3):
                a1[t, p, pl.ds(y, 8), :] = merged_rows(y, t, p, 2) * (1.0 / 64.0)
        return carry

    lax.fori_loop(0, steps, level_one_merge, 0)

    def level_zero(j, carry):
        detail_step(pl.multiple_of(j * 8, 8), lo0, hi0, 1, 0, 2, planes + 2, a1)
        return carry

    lax.fori_loop(0, steps, level_zero, 0)

    def level_zero_merge(j, carry):
        y = pl.multiple_of(j * 8, 8)
        for t in range(2):
            for p in range(planes):
                value = a0[t, 1 + margin + p, pl.ds(y, 8), :] - merged_rows(y, t, margin + p, 1) * (1.0 / 64.0)
                mixed[t, pl.ds(y * planes + p, 8, stride=planes), :] = value
        return carry

    lax.fori_loop(0, steps, level_zero_merge, 0)
    for t in range(2):
        kept = mixed[t, edge * planes : (rows - edge) * planes].astype(out_ref.dtype)
        for copy in range(out_ref.shape[0]):
            out_ref[copy, t] = kept


def whole(array):
    shape = array.shape
    return pl.BlockSpec(shape, lambda *_: (0,) * len(shape))


def shrink(row, chip, halo, thresholds, edge, copies):
    _, chip_planes, rows, width = chip.shape
    planes = chip_planes // 2
    margin = halo.shape[1]
    count = planes + 2 * margin
    scale = np.array([[2.0 ** (1.5 * (level + 1))] for level in range(thresholds.shape[0])], np.float32)
    limits = thresholds * scale
    f32 = jnp.float32
    buffers = [
        pltpu.VMEM((2, chip_planes + planes, rows, width), f32),
        pltpu.VMEM((2, count, rows + 8, width), f32),
        pltpu.VMEM((2, count, rows + 8, width), f32),
        pltpu.VMEM((2, count, rows, width), f32),
        pltpu.VMEM((2, count, rows + 8, width), f32),
        pltpu.VMEM((2, count, rows + 8, width), f32),
        pltpu.VMEM((2, 2, count, rows, width), f32),
        pltpu.VMEM((2, 2, count, rows + 8, width), f32),
        pltpu.VMEM((2, rows * planes, width), f32),
    ]

    def kernel(*refs):
        wavelet_kernel(edge, margin, *refs)

    return pl.pallas_call(
        kernel,
        out_shape=jax.ShapeDtypeStruct((copies, 2, (rows - 2 * edge) * planes, width), jnp.bfloat16),
        in_specs=[
            pl.BlockSpec(memory_space=pltpu.SMEM),
            pl.BlockSpec(memory_space=pltpu.VMEM),
            pl.BlockSpec(memory_space=pltpu.VMEM),
            pl.BlockSpec(memory_space=pltpu.SMEM),
        ],
        out_specs=pl.BlockSpec(memory_space=pltpu.VMEM),
        scratch_shapes=buffers,
        name="wavelet",
    )(row, chip, halo, limits)


def local(image, sens, measured, mask, thresholds):
    _, phase_cells, planes, width = image.shape
    coils = sens.shape[1]
    own_lines, depth_cells = measured.shape[2], measured.shape[3]
    slabs, rows, columns = (lax.axis_size(name) for name in ("slab", "row", "coil"))
    row = lax.axis_index("row")
    lines = own_lines * rows
    group = lines * planes
    half = coils // rows
    bf16, f32 = jnp.bfloat16, jnp.float32
    other = [(0, 1), (1, 0)]

    order = (np.arange(slabs)[None, :] * lines + np.arange(lines)[:, None]).reshape(-1)
    depth_order = np.arange(depth_cells).reshape(slabs, rows, planes).transpose(1, 0, 2).reshape(-1)
    table_phase = fourier_table(phase_cells, -1.0, rows=order)
    inverse_phase = fourier_table(phase_cells, 1.0, columns=order)
    table_depth = fourier_table(depth_cells, -1.0, columns=depth_order)
    inverse_depth = fourier_table(depth_cells, 1.0, rows=depth_order)
    inverse_readout = fourier_table(width, 1.0).T.reshape(2, width, 2, width)

    image_rows = image.reshape(2, phase_cells * planes, width)
    sens_rows = sens.reshape(2, coils, phase_cells * planes, width)
    sens_spec = (2, 1, phase_cells * planes, width)
    piece = (slabs, 2, half, group, width)
    exchanged = jax.ShapeDtypeStruct((slabs, rows, 2, half, group, width), bf16)
    stack = pltpu.VMEM((2, phase_cells * planes, width), f32)
    here = row.astype(jnp.int32).reshape(1)

    def given(kernel, grid_spec, out_shape, name):
        return pl.pallas_call(kernel, grid_spec=grid_spec, out_shape=out_shape, name=name)

    def send_kernel(_, *refs):
        forward_kernel(slabs, lines, planes, *refs)

    sent = given(
        send_kernel,
        pltpu.PrefetchScalarGridSpec(
            num_scalar_prefetch=1,
            grid=(half,),
            in_specs=[
                pl.BlockSpec(sens_spec, lambda c, r: (0, (1 - r[0]) * half + c, 0, 0)),
                whole(image_rows),
                whole(table_phase),
            ],
            out_specs=pl.BlockSpec((slabs, 2, 1, group, width), lambda c, r: (0, 0, c, 0, 0)),
            scratch_shapes=[stack, stack],
        ),
        jax.ShapeDtypeStruct(piece, bf16),
        "forward_sent",
    )(here, sens_rows, image_rows, table_phase)
    arrived = lax.ppermute(sent, "row", other)

    def keep_kernel(_, sens_ref, image_ref, table_ref, out_ref, product, mixed):
        forward_kernel(slabs, lines, planes, sens_ref, image_ref, table_ref, out_ref.at[:, 0], product, mixed)

    kept = given(
        keep_kernel,
        pltpu.PrefetchScalarGridSpec(
            num_scalar_prefetch=1,
            grid=(half,),
            in_specs=[
                pl.BlockSpec(sens_spec, lambda c, r: (0, r[0] * half + c, 0, 0)),
                whole(image_rows),
                whole(table_phase),
            ],
            out_specs=pl.BlockSpec((slabs, 1, 2, 1, group, width), lambda c, r: (0, 0, 0, c, 0, 0)),
            scratch_shapes=[stack, stack],
        ),
        exchanged,
        "forward_kept",
    )(here, sens_rows, image_rows, table_phase)

    def place_kernel(r_ref, _, arrived_ref, out_ref, pause_ref):
        @pl.when(pl.program_id(0) == 0)
        def _():
            pause_ref[...] = lax.fori_loop(
                0, r_ref[0] * pause_steps, lambda _, v: v * 1.0001 + 0.5, jnp.ones(pause_ref.shape, jnp.float32)
            )

        out_ref[:, 0] = arrived_ref[...]

    pieces = 4
    outgoing, _ = pl.pallas_call(
        place_kernel,
        grid_spec=pltpu.PrefetchScalarGridSpec(
            num_scalar_prefetch=1,
            grid=(pieces,),
            in_specs=[
                pl.BlockSpec(memory_space=pl.ANY),
                pl.BlockSpec((slabs // pieces, 2, half, group, width), lambda i, r: (i, 0, 0, 0, 0)),
            ],
            out_specs=[
                pl.BlockSpec((slabs // pieces, 1, 2, half, group, width), lambda i, r: (i, 1, 0, 0, 0, 0)),
                pl.BlockSpec((8, 128), lambda i, r: (0, 0)),
            ],
        ),
        out_shape=[exchanged, jax.ShapeDtypeStruct((8, 128), f32)],
        input_output_aliases={1: 0},
        name="place",
    )(here, kept, arrived)

    received = lax.all_to_all(outgoing, "slab", 0, 0, tiled=True)

    measured, mask, sens_late, image, _ = lax.optimization_barrier((measured, mask, sens_rows, image, outgoing))

    def both_rows(values, axis):
        kept = lax.dynamic_slice_in_dim(values, row * half, half, axis=1)
        away = lax.dynamic_slice_in_dim(values, (1 - row) * half, half, axis=1)
        return in_row_order(kept, lax.ppermute(away, "row", other), axis)

    def in_row_order(own, others, axis):
        first = row == 0
        return jnp.concatenate([jnp.where(first, own, others), jnp.where(first, others, own)], axis=axis)

    own_measured = jnp.einsum(
        "tclzk,tksx->sclzx", measured, inverse_readout, preferred_element_type=f32
    ).astype(bf16)
    chip_measured = both_rows(own_measured, 2)
    own_mask = mask.astype(f32)
    chip_mask = in_row_order(own_mask, lax.ppermute(own_mask, "row", other), 0)
    wide_mask = jnp.broadcast_to(chip_mask[:, :, None], (lines, depth_cells, width))
    chip_sens = both_rows(sens_late[:, :, None], 2)
    edge = 4
    quarter = phase_cells // columns
    image_planes = jnp.transpose(image, (0, 2, 1, 3))
    framed = jnp.concatenate(
        [image_planes[:, :, phase_cells - edge :], image_planes, image_planes[:, :, :edge]], axis=2
    )
    own_image = lax.dynamic_slice_in_dim(
        framed, lax.axis_index("coil") * quarter, quarter + 2 * edge, axis=2
    )
    chip_image = in_row_order(own_image, lax.ppermute(own_image, "row", other), 1)

    def mid_kernel(_, *refs):
        middle_kernel(lines, *refs)

    block = (slabs, 1, 2, 1, group, width)
    buffer = pltpu.VMEM((rows, 2, slabs * group, width), f32)
    returning = given(
        mid_kernel,
        pltpu.PrefetchScalarGridSpec(
            num_scalar_prefetch=1,
            grid=(half,),
            in_specs=[
                pl.BlockSpec(block, lambda c, r: (0, r[0], 0, c, 0, 0)),
                pl.BlockSpec(block, lambda c, r: (0, 1 - r[0], 0, c, 0, 0)),
                pl.BlockSpec((2, 1, lines, depth_cells, width), lambda c, r: (0, c, 0, 0, 0)),
                whole(wide_mask),
                whole(table_depth),
                whole(inverse_depth),
            ],
            out_specs=pl.BlockSpec((slabs, rows, 2, 1, group, width), lambda c, r: (0, 0, 0, c, 0, 0)),
            scratch_shapes=[buffer, buffer],
        ),
        exchanged,
        "middle",
    )(here, received, received, chip_measured, wide_mask, table_depth, inverse_depth)
    returned = lax.all_to_all(returning, "slab", 0, 0, tiled=True)
    returned, chip_image = lax.optimization_barrier((returned, chip_image))

    tall = quarter + 2 * edge

    def back_kernel(*refs):
        backward_kernel(lines, planes, edge, *refs)

    parts = pl.pallas_call(
        back_kernel,
        grid=(half,),
        out_shape=jax.ShapeDtypeStruct((columns, 2, rows * planes, tall, width), bf16),
        in_specs=[
            pl.BlockSpec((slabs, rows, 2, 1, group, width), lambda c: (0, 0, 0, c, 0, 0)),
            pl.BlockSpec((2, 1, rows, phase_cells * planes, width), lambda c: (0, c, 0, 0, 0)),
            whole(inverse_phase),
        ],
        out_specs=pl.BlockSpec((columns, 2, rows * planes, tall, width), lambda c: (0, 0, 0, 0, 0)),
        scratch_shapes=[
            buffer,
            buffer,
            pltpu.VMEM((rows, 2, planes, phase_cells, width), f32),
            pltpu.VMEM((phase_cells + 2 * edge, width), f32),
        ],
        name="backward",
    )(returned, chip_sens, inverse_phase)
    share = lax.all_to_all(parts, "coil", 0, 0, tiled=True).astype(f32).sum(axis=0)
    others = lax.ppermute(share.astype(bf16), "row", other)
    chip = chip_image - step_size * (share + others.astype(f32))
    margin = 2 ** thresholds.shape[0] - 1
    last = rows * planes - margin
    edge_planes = lax.dynamic_slice_in_dim(chip, row * last, margin, axis=1).astype(bf16)
    pairs = []
    for slab in range(slabs):
        after = (slab + 1) % slabs
        pairs.append((slab * rows + rows - 1, after * rows))
        pairs.append((after * rows, slab * rows + rows - 1))
    halo = lax.ppermute(edge_planes, lines_axes, pairs)
    result = shrink(here, chip, halo, thresholds, edge, columns)
    gathered = lax.all_to_all(result, "coil", 0, 0, tiled=True)
    result_rows = jnp.swapaxes(gathered, 0, 1).reshape(2, phase_cells * planes, width)
    return result_rows.astype(f32).reshape(2, phase_cells, planes, width)


def solution(mesh):
    return jax.shard_map(
        local,
        mesh=mesh,
        in_specs=(
            P("groups", None, lines_axes, None),
            P("groups", "coil", None, lines_axes, None),
            P("groups", "coil", lines_axes, None, None),
            P(lines_axes, None),
            P(),
        ),
        out_specs=P("groups", None, lines_axes, None),
        check_vma=False,
    )
```

```python
import math

import jax
import jax.numpy as jnp
import ml_dtypes
import numpy as np
from jax import lax
from jax.experimental import pallas as pl
from jax.experimental.pallas import tpu as pltpu
from jax.sharding import PartitionSpec as P

step_size = 0.5
lines_axes = ("slab", "row")
pause_steps = 6500


def fourier_table(length, sign, rows=None, columns=None):
    index = np.arange(length, dtype=np.int64)
    phase = (index[:, None] * index[None, :]) % length
    theta = phase.astype(np.float32) * np.float32(2.0 * math.pi / length)
    scale = np.float32(1.0 / math.sqrt(length))
    real = (np.cos(theta) * scale).astype(np.float32)
    imaginary = (np.sin(theta) * np.float32(sign) * scale).astype(np.float32)
    if rows is not None:
        real, imaginary = real[rows], imaginary[rows]
    if columns is not None:
        real, imaginary = real[:, columns], imaginary[:, columns]
    return np.block([[real, -imaginary], [imaginary, real]]).astype(ml_dtypes.bfloat16)


def dot(left, right):
    return jnp.dot(left, right, preferred_element_type=jnp.float32)


def forward_kernel(slabs, lines, planes, coil, sens_ref, image_ref, table_ref, out_ref, product, mixed):
    cells = product.shape[1] // planes
    group = lines * planes
    sr = sens_ref[0, 0].astype(jnp.float32)
    si = sens_ref[1, 0].astype(jnp.float32)
    ir = image_ref[0]
    ii = image_ref[1]
    product[0] = sr * ir - si * ii
    product[1] = sr * ii + si * ir
    columns = [
        jnp.concatenate(
            [product[t, pl.ds(z, cells, stride=planes), :].astype(jnp.bfloat16) for t in range(2)],
            axis=0,
        )
        for z in range(planes)
    ]
    done = dot(table_ref[...], jnp.concatenate(columns, axis=1))
    width = product.shape[2]
    for s in range(2):
        for z in range(planes):
            for line in range(lines):
                first = s * cells + line * slabs
                mixed[s, pl.ds(z * lines + line, slabs, stride=group), :] = done[
                    first : first + slabs, z * width : (z + 1) * width
                ]
        out_ref[:, s, coil] = mixed[s].astype(jnp.bfloat16).reshape(slabs, group, width)


def middle_kernel(lines, row_ref, in_ref, measured_ref, mask_ref, table_ref, inverse_ref, out_ref, mixed, back):
    slabs, _, _, _, group, width = in_ref.shape
    half = slabs * group // lines
    cells = 2 * half
    coil = pl.program_id(0)
    for row in range(2):
        place = row_ref[0] if row == 0 else 1 - row_ref[0]
        for t in range(2):
            mixed[row, t] = in_ref[:, place, t, coil].astype(jnp.float32).reshape(slabs * group, width)
    columns = [
        jnp.concatenate(
            [
                mixed[row, t, pl.ds(line, half, stride=lines), :].astype(jnp.bfloat16)
                for t in range(2)
                for row in range(2)
            ],
            axis=0,
        )
        for line in range(lines)
    ]
    spectrum = dot(table_ref[...], jnp.concatenate(columns, axis=1))
    residual = []
    for line in range(lines):
        parts = []
        for t in range(2):
            value = spectrum[t * cells : (t + 1) * cells, line * width : (line + 1) * width]
            value = mask_ref[line] * (value - measured_ref[t, coil, line].astype(jnp.float32))
            parts.append(value.astype(jnp.bfloat16))
        residual.append(jnp.concatenate(parts, axis=0))
    result = dot(inverse_ref[...], jnp.concatenate(residual, axis=1))
    for row in range(2):
        for s in range(2):
            first = s * cells + row * half
            for line in range(lines):
                back[row, s, pl.ds(line, half, stride=lines), :] = result[
                    first : first + half, line * width : (line + 1) * width
                ]
            out_ref[:, row, s, 0] = back[row, s].astype(jnp.bfloat16).reshape(slabs, group, width)


def backward_kernel(lines, planes, edge, in_ref, sens_ref, table_ref, out_ref, mixed, wide, total, framed):
    slabs, rows, _, _, group, width = in_ref.shape
    cells = slabs * lines
    coil = pl.program_id(0)

    @pl.when(coil == 0)
    def _():
        total[...] = jnp.zeros(total.shape, jnp.float32)

    for row in range(rows):
        for t in range(2):
            mixed[row, t] = in_ref[:, row, t, coil].astype(jnp.float32).reshape(slabs * group, width)
            wide[row, t] = sens_ref[t, coil, row].astype(jnp.float32)
    columns = [
        jnp.concatenate(
            [
                mixed[row, t, pl.ds(z * lines + line, slabs, stride=group), :].astype(jnp.bfloat16)
                for t in range(2)
                for line in range(lines)
            ],
            axis=0,
        )
        for row in range(rows)
        for z in range(planes)
    ]
    done = dot(table_ref[...], jnp.concatenate(columns, axis=1))
    for row in range(rows):
        for z in range(planes):
            plane = row * planes + z
            rr = done[:cells, plane * width : (plane + 1) * width]
            ri = done[cells:, plane * width : (plane + 1) * width]
            sr = wide[row, 0, pl.ds(z, cells, stride=planes), :]
            si = wide[row, 1, pl.ds(z, cells, stride=planes), :]
            total[row, 0, z] += sr * rr + si * ri
            total[row, 1, z] += sr * ri - si * rr

    @pl.when(coil == pl.num_programs(0) - 1)
    def _():
        pieces, _, _, tall, _ = out_ref.shape
        step = tall - 2 * edge
        for row in range(rows):
            for t in range(2):
                for z in range(planes):
                    framed[0:edge] = total[row, t, z, cells - edge : cells]
                    framed[edge : edge + cells] = total[row, t, z]
                    framed[edge + cells :] = total[row, t, z, 0:edge]
                    for q in range(pieces):
                        out_ref[q, t, row * planes + z] = framed[q * step : q * step + tall].astype(out_ref.dtype)


def removed(real, imaginary, limit):
    factor = jnp.minimum(lax.rsqrt(real * real + imaginary * imaginary) * limit, 1.0)
    return real * factor, imaginary * factor


def wavelet_kernel(edge, margin, row_ref, chip_ref, halo_ref, limits_ref, out_ref, a0, lo0, hi0, a1, lo1, hi1, sums, diffs, mixed):
    chip_planes, rows, width = chip_ref.shape[1:]
    planes = chip_planes // 2
    count = planes + 2 * margin
    steps = rows // 8
    pad = 8
    row = row_ref[0]
    for t in range(2):
        for p in range(chip_planes):
            a0[t, (1 - row) * planes + p] = chip_ref[t, p]
        for p in range(margin):
            a0[t, 1 + row * (margin + planes) + p] = halo_ref[t, p].astype(jnp.float32)

    def split_lanes(source, shift, lo, hi, lo_planes, hi_planes, offset):
        def step(j, carry):
            y = pl.multiple_of(j * 8, 8)
            for t in range(2):
                for p in lo_planes:
                    v = source[t, p + shift, pl.ds(y, 8), :]
                    s = pltpu.roll(v, width - offset, 1)
                    lo[t, p, pl.ds(y, 8), :] = v + s
                    if p in hi_planes:
                        hi[t, p, pl.ds(y, 8), :] = v - s
            return carry

        lax.fori_loop(0, steps, step, 0)

    def detail_step(y, lo, hi, offset, level, first, last, coarse):
        for x_band, source in ((0, lo), (1, hi)):
            merged = []
            for y_band in range(2):
                band = x_band + 2 * y_band
                v = {}
                for p in range(first, last + offset + 1):
                    for t in range(2):
                        here = source[t, p, pl.ds(y, 8), :]
                        there = source[t, p, pl.ds(y + offset, 8), :]
                        v[p, t] = here + there if y_band == 0 else here - there
                plus, minus = {}, {}
                for p in range(first, last + 1):
                    high = removed(
                        v[p, 0] - v[p + offset, 0], v[p, 1] - v[p + offset, 1], limits_ref[level, band + 3]
                    )
                    if band:
                        low = removed(
                            v[p, 0] + v[p + offset, 0], v[p, 1] + v[p + offset, 1], limits_ref[level, band - 1]
                        )
                    elif coarse is not None:
                        low = (coarse[0, p, pl.ds(y, 8), :], coarse[1, p, pl.ds(y, 8), :])
                    else:
                        low = None
                    for t in range(2):
                        plus[p, t] = high[t] if low is None else low[t] + high[t]
                        minus[p, t] = -high[t] if low is None else low[t] - high[t]
                merged.append(
                    {
                        (p, t): plus[p, t] + minus[p - offset, t]
                        for p in range(first + offset, last + 1)
                        for t in range(2)
                    }
                )
            for p, t in merged[0]:
                sums[x_band, t, p, pl.ds(y, 8), :] = merged[0][p, t] + merged[1][p, t]
                diffs[x_band, t, p, pl.ds(y + pad, 8), :] = merged[0][p, t] - merged[1][p, t]

    def merged_rows(y, t, p, offset):
        lower = sums[0, t, p, pl.ds(y, 8), :] + diffs[0, t, p, pl.ds(y + pad - offset, 8), :]
        upper = sums[1, t, p, pl.ds(y, 8), :] + diffs[1, t, p, pl.ds(y + pad - offset, 8), :]
        return lower + upper + pltpu.roll(lower - upper, offset, 1)

    split_lanes(a0, 1, lo0, hi0, range(count), range(2, planes + 4), 1)

    def coarse_step(j, carry):
        y = pl.multiple_of(j * 8, 8)
        for t in range(2):
            v = [lo0[t, p, pl.ds(y, 8), :] + lo0[t, p, pl.ds(y + 1, 8), :] for p in range(count)]
            for p in range(count - 1):
                w = v[p] + v[p + 1]
                a1[t, p, pl.ds(y, 8), :] = w
        return carry

    lax.fori_loop(0, steps, coarse_step, 0)

    split_lanes(a1, 0, lo1, hi1, range(count - 1), range(count - 1), 2)

    def level_one(j, carry):
        detail_step(pl.multiple_of(j * 8, 8), lo1, hi1, 2, 1, 0, planes + 2, None)
        return carry

    lax.fori_loop(0, steps, level_one, 0)

    def level_one_merge(j, carry):
        y = pl.multiple_of(j * 8, 8)
        for t in range(2):
            for p in range(2, planes + 3):
                a1[t, p, pl.ds(y, 8), :] = merged_rows(y, t, p, 2) * (1.0 / 64.0)
        return carry

    lax.fori_loop(0, steps, level_one_merge, 0)

    def level_zero(j, carry):
        detail_step(pl.multiple_of(j * 8, 8), lo0, hi0, 1, 0, 2, planes + 2, a1)
        return carry

    lax.fori_loop(0, steps, level_zero, 0)

    def level_zero_merge(j, carry):
        y = pl.multiple_of(j * 8, 8)
        for t in range(2):
            for p in range(planes):
                value = a0[t, 1 + margin + p, pl.ds(y, 8), :] - merged_rows(y, t, margin + p, 1) * (1.0 / 64.0)
                mixed[t, pl.ds(y * planes + p, 8, stride=planes), :] = value
        return carry

    lax.fori_loop(0, steps, level_zero_merge, 0)
    for t in range(2):
        kept = mixed[t, edge * planes : (rows - edge) * planes].astype(out_ref.dtype)
        for copy in range(out_ref.shape[0]):
            out_ref[copy, t] = kept


def resident(array):
    return pltpu.with_memory_space_constraint(array, pltpu.VMEM)


in_place = pl.BlockSpec(memory_space=pltpu.VMEM)


def whole(array):
    shape = array.shape
    return pl.BlockSpec(shape, lambda *_: (0,) * len(shape))


def shrink(row, chip, halo, thresholds, edge, copies):
    _, chip_planes, rows, width = chip.shape
    planes = chip_planes // 2
    margin = halo.shape[1]
    count = planes + 2 * margin
    scale = np.array([[2.0 ** (1.5 * (level + 1))] for level in range(thresholds.shape[0])], np.float32)
    limits = thresholds * scale
    f32 = jnp.float32
    buffers = [
        pltpu.VMEM((2, chip_planes + planes, rows, width), f32),
        pltpu.VMEM((2, count, rows + 8, width), f32),
        pltpu.VMEM((2, count, rows + 8, width), f32),
        pltpu.VMEM((2, count, rows, width), f32),
        pltpu.VMEM((2, count, rows + 8, width), f32),
        pltpu.VMEM((2, count, rows + 8, width), f32),
        pltpu.VMEM((2, 2, count, rows, width), f32),
        pltpu.VMEM((2, 2, count, rows + 8, width), f32),
        pltpu.VMEM((2, rows * planes, width), f32),
    ]

    def kernel(*refs):
        wavelet_kernel(edge, margin, *refs)

    return pl.pallas_call(
        kernel,
        out_shape=pltpu.VMEM((copies, 2, (rows - 2 * edge) * planes, width), jnp.bfloat16),
        in_specs=[
            pl.BlockSpec(memory_space=pltpu.SMEM),
            in_place,
            in_place,
            pl.BlockSpec(memory_space=pltpu.SMEM),
        ],
        out_specs=pl.BlockSpec(memory_space=pltpu.VMEM),
        scratch_shapes=buffers,
        name="wavelet",
    )(row, resident(chip), resident(halo), limits)


def local(image, sens, measured, mask, thresholds):
    _, phase_cells, planes, width = image.shape
    coils = sens.shape[1]
    own_lines, depth_cells = measured.shape[2], measured.shape[3]
    slabs, rows, columns = (lax.axis_size(name) for name in ("slab", "row", "coil"))
    row = lax.axis_index("row")
    lines = own_lines * rows
    group = lines * planes
    half = coils // rows
    bf16, f32 = jnp.bfloat16, jnp.float32
    other = [(0, 1), (1, 0)]

    order = (np.arange(slabs)[None, :] * lines + np.arange(lines)[:, None]).reshape(-1)
    depth_order = np.arange(depth_cells).reshape(slabs, rows, planes).transpose(1, 0, 2).reshape(-1)
    table_phase = fourier_table(phase_cells, -1.0, rows=order)
    inverse_phase = fourier_table(phase_cells, 1.0, columns=order)
    table_depth = fourier_table(depth_cells, -1.0, columns=depth_order)
    inverse_depth = fourier_table(depth_cells, 1.0, rows=depth_order)
    inverse_readout = fourier_table(width, 1.0).T.reshape(2, width, 2, width)

    image_rows = image.reshape(2, phase_cells * planes, width)
    sens_rows = sens.reshape(2, coils, phase_cells * planes, width)
    sens_spec = (2, 1, phase_cells * planes, width)
    piece = (slabs, 2, half, group, width)
    exchanged = jax.ShapeDtypeStruct((slabs, rows, 2, half, group, width), bf16)
    stack = pltpu.VMEM((2, phase_cells * planes, width), f32)
    here = row.astype(jnp.int32).reshape(1)

    def given(kernel, grid_spec, out_shape, name):
        return pl.pallas_call(kernel, grid_spec=grid_spec, out_shape=out_shape, name=name)

    def send_kernel(_, *refs):
        forward_kernel(slabs, lines, planes, pl.program_id(0), *refs)

    sent = given(
        send_kernel,
        pltpu.PrefetchScalarGridSpec(
            num_scalar_prefetch=1,
            grid=(half,),
            in_specs=[
                pl.BlockSpec(sens_spec, lambda c, r: (0, (1 - r[0]) * half + c, 0, 0)),
                whole(image_rows),
                whole(table_phase),
            ],
            out_specs=in_place,
            scratch_shapes=[stack, stack],
        ),
        pltpu.VMEM(piece, bf16),
        "forward_sent",
    )(here, sens_rows, image_rows, table_phase)
    arrived = lax.ppermute(sent, "row", other)

    def keep_kernel(_, sens_ref, image_ref, table_ref, out_ref, product, mixed):
        forward_kernel(slabs, lines, planes, 0, sens_ref, image_ref, table_ref, out_ref.at[:, 0], product, mixed)

    kept = given(
        keep_kernel,
        pltpu.PrefetchScalarGridSpec(
            num_scalar_prefetch=1,
            grid=(half,),
            in_specs=[
                pl.BlockSpec(sens_spec, lambda c, r: (0, r[0] * half + c, 0, 0)),
                whole(image_rows),
                whole(table_phase),
            ],
            out_specs=pl.BlockSpec((slabs, 1, 2, 1, group, width), lambda c, r: (0, 0, 0, c, 0, 0)),
            scratch_shapes=[stack, stack],
        ),
        exchanged,
        "forward_kept",
    )(here, sens_rows, image_rows, table_phase)

    def place_kernel(r_ref, _, arrived_ref, out_ref, pause_ref, done):
        copy = pltpu.make_async_copy(arrived_ref, out_ref.at[:, 1], done)
        copy.start()
        pause_ref[...] = lax.fori_loop(
            0, r_ref[0] * pause_steps, lambda _, v: v * 1.0001 + 0.5, jnp.ones(pause_ref.shape, jnp.float32)
        )
        copy.wait()

    outgoing, _ = pl.pallas_call(
        place_kernel,
        in_specs=[
            pl.BlockSpec(memory_space=pltpu.SMEM),
            pl.BlockSpec(memory_space=pl.ANY),
            in_place,
        ],
        out_specs=[pl.BlockSpec(memory_space=pl.ANY), pl.BlockSpec(memory_space=pltpu.VMEM)],
        out_shape=[exchanged, jax.ShapeDtypeStruct((8, 128), f32)],
        scratch_shapes=[pltpu.SemaphoreType.DMA],
        input_output_aliases={1: 0},
        name="place",
    )(here, kept, resident(arrived))

    received = lax.all_to_all(outgoing, "slab", 0, 0, tiled=True)

    measured, mask, sens_late, image, _ = lax.optimization_barrier((measured, mask, sens_rows, image, outgoing))

    def both_rows(values, axis):
        kept = lax.dynamic_slice_in_dim(values, row * half, half, axis=1)
        away = lax.dynamic_slice_in_dim(values, (1 - row) * half, half, axis=1)
        return in_row_order(kept, lax.ppermute(away, "row", other), axis)

    def in_row_order(own, others, axis):
        first = row == 0
        return jnp.concatenate([jnp.where(first, own, others), jnp.where(first, others, own)], axis=axis)

    own_measured = jnp.einsum(
        "tclzk,tksx->sclzx", measured, inverse_readout, preferred_element_type=f32
    ).astype(bf16)
    chip_measured = both_rows(own_measured, 2)
    own_mask = mask.astype(f32)
    chip_mask = in_row_order(own_mask, lax.ppermute(own_mask, "row", other), 0)
    wide_mask = jnp.broadcast_to(chip_mask[:, :, None], (lines, depth_cells, width))
    chip_sens = both_rows(sens_late[:, :, None], 2)
    edge = 4
    quarter = phase_cells // columns
    image_planes = jnp.transpose(image, (0, 2, 1, 3))
    framed = jnp.concatenate(
        [image_planes[:, :, phase_cells - edge :], image_planes, image_planes[:, :, :edge]], axis=2
    )
    own_image = lax.dynamic_slice_in_dim(
        framed, lax.axis_index("coil") * quarter, quarter + 2 * edge, axis=2
    )
    chip_image = in_row_order(own_image, lax.ppermute(own_image, "row", other), 1)

    def mid_kernel(*refs):
        middle_kernel(lines, *refs)

    buffer = pltpu.VMEM((rows, 2, slabs * group, width), f32)
    returning = given(
        mid_kernel,
        pltpu.PrefetchScalarGridSpec(
            num_scalar_prefetch=1,
            grid=(half,),
            in_specs=[
                in_place,
                in_place,
                in_place,
                whole(table_depth),
                whole(inverse_depth),
            ],
            out_specs=pl.BlockSpec((slabs, rows, 2, 1, group, width), lambda c, r: (0, 0, 0, c, 0, 0)),
            scratch_shapes=[buffer, buffer],
        ),
        exchanged,
        "middle",
    )(here, *map(resident, (received, chip_measured, wide_mask)), table_depth, inverse_depth)
    returned = lax.all_to_all(returning, "slab", 0, 0, tiled=True)
    returned, chip_image = lax.optimization_barrier((returned, chip_image))

    tall = quarter + 2 * edge

    def back_kernel(*refs):
        backward_kernel(lines, planes, edge, *refs)

    parts = pl.pallas_call(
        back_kernel,
        grid=(half,),
        out_shape=pltpu.VMEM((columns, 2, rows * planes, tall, width), bf16),
        in_specs=[in_place, in_place, whole(inverse_phase)],
        out_specs=in_place,
        scratch_shapes=[
            buffer,
            buffer,
            pltpu.VMEM((rows, 2, planes, phase_cells, width), f32),
            pltpu.VMEM((phase_cells + 2 * edge, width), f32),
        ],
        name="backward",
    )(resident(returned), resident(chip_sens), inverse_phase)
    share = lax.all_to_all(parts, "coil", 0, 0, tiled=True).astype(f32).sum(axis=0)
    others = lax.ppermute(share.astype(bf16), "row", other)
    chip = chip_image - step_size * (share + others.astype(f32))
    margin = 2 ** thresholds.shape[0] - 1
    last = rows * planes - margin
    edge_planes = lax.dynamic_slice_in_dim(chip, row * last, margin, axis=1).astype(bf16)
    pairs = []
    for slab in range(slabs):
        after = (slab + 1) % slabs
        pairs.append((slab * rows + rows - 1, after * rows))
        pairs.append((after * rows, slab * rows + rows - 1))
    halo = lax.ppermute(edge_planes, lines_axes, pairs)
    result = shrink(here, chip, halo, thresholds, edge, columns)
    gathered = lax.all_to_all(result, "coil", 0, 0, tiled=True)
    result_rows = jnp.swapaxes(gathered, 0, 1).reshape(2, phase_cells * planes, width)
    return result_rows.astype(f32).reshape(2, phase_cells, planes, width)


def solution(mesh):
    return jax.shard_map(
        local,
        mesh=mesh,
        in_specs=(
            P("groups", None, lines_axes, None),
            P("groups", "coil", None, lines_axes, None),
            P("groups", "coil", lines_axes, None, None),
            P(lines_axes, None),
            P(),
        ),
        out_specs=P("groups", None, lines_axes, None),
        check_vma=False,
    )
```

```python
import math

import jax
import jax.numpy as jnp
import ml_dtypes
import numpy as np
from jax import lax
from jax.experimental import pallas as pl
from jax.experimental.pallas import tpu as pltpu
from jax.sharding import PartitionSpec as P

step_size = 0.5
lines_axes = ("slab", "row")
pause_steps = 7100


def fourier_table(length, sign, rows=None, columns=None):
    index = np.arange(length, dtype=np.int64)
    phase = (index[:, None] * index[None, :]) % length
    theta = phase.astype(np.float32) * np.float32(2.0 * math.pi / length)
    scale = np.float32(1.0 / math.sqrt(length))
    real = (np.cos(theta) * scale).astype(np.float32)
    imaginary = (np.sin(theta) * np.float32(sign) * scale).astype(np.float32)
    if rows is not None:
        real, imaginary = real[rows], imaginary[rows]
    if columns is not None:
        real, imaginary = real[:, columns], imaginary[:, columns]
    return np.block([[real, -imaginary], [imaginary, real]]).astype(ml_dtypes.bfloat16)


def dot(left, right):
    return jnp.dot(left, right, preferred_element_type=jnp.float32)


def forward_kernel(slabs, lines, planes, coil, sens_ref, image_ref, table_ref, out_ref, product, mixed):
    cells = product.shape[1] // planes
    group = lines * planes
    sr = sens_ref[0, 0].astype(jnp.float32)
    si = sens_ref[1, 0].astype(jnp.float32)
    ir = image_ref[0]
    ii = image_ref[1]
    product[0] = sr * ir - si * ii
    product[1] = sr * ii + si * ir
    columns = [
        jnp.concatenate(
            [product[t, pl.ds(z, cells, stride=planes), :].astype(jnp.bfloat16) for t in range(2)],
            axis=0,
        )
        for z in range(planes)
    ]
    done = dot(table_ref[...], jnp.concatenate(columns, axis=1))
    width = product.shape[2]
    for s in range(2):
        for z in range(planes):
            for line in range(lines):
                first = s * cells + line * slabs
                mixed[s, pl.ds(z * lines + line, slabs, stride=group), :] = done[
                    first : first + slabs, z * width : (z + 1) * width
                ]
        out_ref[:, s, coil] = mixed[s].astype(jnp.bfloat16).reshape(slabs, group, width)


def middle_kernel(lines, row_ref, in_ref, measured_ref, mask_ref, table_ref, inverse_ref, out_ref, mixed, back):
    slabs, _, _, _, group, width = in_ref.shape
    half = slabs * group // lines
    cells = 2 * half
    coil = pl.program_id(0)
    for row in range(2):
        place = row_ref[0] if row == 0 else 1 - row_ref[0]
        for t in range(2):
            mixed[row, t] = in_ref[:, place, t, coil].astype(jnp.float32).reshape(slabs * group, width)
    columns = [
        jnp.concatenate(
            [
                mixed[row, t, pl.ds(line, half, stride=lines), :].astype(jnp.bfloat16)
                for t in range(2)
                for row in range(2)
            ],
            axis=0,
        )
        for line in range(lines)
    ]
    spectrum = dot(table_ref[...], jnp.concatenate(columns, axis=1))
    residual = []
    for line in range(lines):
        parts = []
        for t in range(2):
            value = spectrum[t * cells : (t + 1) * cells, line * width : (line + 1) * width]
            value = mask_ref[line] * (value - measured_ref[t, coil, line].astype(jnp.float32))
            parts.append(value.astype(jnp.bfloat16))
        residual.append(jnp.concatenate(parts, axis=0))
    result = dot(inverse_ref[...], jnp.concatenate(residual, axis=1))
    for row in range(2):
        for s in range(2):
            first = s * cells + row * half
            for line in range(lines):
                back[row, s, pl.ds(line, half, stride=lines), :] = result[
                    first : first + half, line * width : (line + 1) * width
                ]
            out_ref[:, row, s, 0] = back[row, s].astype(jnp.bfloat16).reshape(slabs, group, width)


def backward_kernel(lines, planes, edge, in_ref, sens_ref, table_ref, out_ref, mixed, wide, total, framed):
    slabs, rows, _, _, group, width = in_ref.shape
    cells = slabs * lines
    coil = pl.program_id(0)

    @pl.when(coil == 0)
    def _():
        total[...] = jnp.zeros(total.shape, jnp.float32)

    for row in range(rows):
        for t in range(2):
            mixed[row, t] = in_ref[:, row, t, coil].astype(jnp.float32).reshape(slabs * group, width)
            wide[row, t] = sens_ref[t, coil, row].astype(jnp.float32)
    columns = [
        jnp.concatenate(
            [
                mixed[row, t, pl.ds(z * lines + line, slabs, stride=group), :].astype(jnp.bfloat16)
                for t in range(2)
                for line in range(lines)
            ],
            axis=0,
        )
        for row in range(rows)
        for z in range(planes)
    ]
    done = dot(table_ref[...], jnp.concatenate(columns, axis=1))
    for row in range(rows):
        for z in range(planes):
            plane = row * planes + z
            rr = done[:cells, plane * width : (plane + 1) * width]
            ri = done[cells:, plane * width : (plane + 1) * width]
            sr = wide[row, 0, pl.ds(z, cells, stride=planes), :]
            si = wide[row, 1, pl.ds(z, cells, stride=planes), :]
            total[row, 0, z] += sr * rr + si * ri
            total[row, 1, z] += sr * ri - si * rr

    @pl.when(coil == pl.num_programs(0) - 1)
    def _():
        pieces, _, _, tall, _ = out_ref.shape
        step = tall - 2 * edge
        for row in range(rows):
            for t in range(2):
                for z in range(planes):
                    framed[0:edge] = total[row, t, z, cells - edge : cells]
                    framed[edge : edge + cells] = total[row, t, z]
                    framed[edge + cells :] = total[row, t, z, 0:edge]
                    for q in range(pieces):
                        out_ref[q, t, row * planes + z] = framed[q * step : q * step + tall].astype(out_ref.dtype)


def removed(real, imaginary, limit):
    factor = jnp.minimum(lax.rsqrt(real * real + imaginary * imaginary) * limit, 1.0)
    return real * factor, imaginary * factor


def wavelet_kernel(edge, margin, row_ref, chip_ref, halo_ref, limits_ref, out_ref, a0, lo0, hi0, a1, lo1, hi1, sums, diffs, mixed):
    chip_planes, rows, width = chip_ref.shape[1:]
    planes = chip_planes // 2
    count = planes + 2 * margin
    steps = rows // 8
    pad = 8
    row = row_ref[0]
    for t in range(2):
        for p in range(chip_planes):
            a0[t, (1 - row) * planes + p] = chip_ref[t, p]
        for p in range(margin):
            a0[t, 1 + row * (margin + planes) + p] = halo_ref[t, p].astype(jnp.float32)

    def split_lanes(source, shift, lo, hi, lo_planes, hi_planes, offset):
        def step(j, carry):
            y = pl.multiple_of(j * 8, 8)
            for t in range(2):
                for p in lo_planes:
                    v = source[t, p + shift, pl.ds(y, 8), :]
                    s = pltpu.roll(v, width - offset, 1)
                    lo[t, p, pl.ds(y, 8), :] = v + s
                    if p in hi_planes:
                        hi[t, p, pl.ds(y, 8), :] = v - s
            return carry

        lax.fori_loop(0, steps, step, 0)

    def detail_step(y, lo, hi, offset, level, first, last, coarse):
        for x_band, source in ((0, lo), (1, hi)):
            merged = []
            for y_band in range(2):
                band = x_band + 2 * y_band
                v = {}
                for p in range(first, last + offset + 1):
                    for t in range(2):
                        here = source[t, p, pl.ds(y, 8), :]
                        there = source[t, p, pl.ds(y + offset, 8), :]
                        v[p, t] = here + there if y_band == 0 else here - there
                plus, minus = {}, {}
                for p in range(first, last + 1):
                    high = removed(
                        v[p, 0] - v[p + offset, 0], v[p, 1] - v[p + offset, 1], limits_ref[level, band + 3]
                    )
                    if band:
                        low = removed(
                            v[p, 0] + v[p + offset, 0], v[p, 1] + v[p + offset, 1], limits_ref[level, band - 1]
                        )
                    elif coarse is not None:
                        low = (coarse[0, p, pl.ds(y, 8), :], coarse[1, p, pl.ds(y, 8), :])
                    else:
                        low = None
                    for t in range(2):
                        plus[p, t] = high[t] if low is None else low[t] + high[t]
                        minus[p, t] = -high[t] if low is None else low[t] - high[t]
                merged.append(
                    {
                        (p, t): plus[p, t] + minus[p - offset, t]
                        for p in range(first + offset, last + 1)
                        for t in range(2)
                    }
                )
            for p, t in merged[0]:
                sums[x_band, t, p, pl.ds(y, 8), :] = merged[0][p, t] + merged[1][p, t]
                diffs[x_band, t, p, pl.ds(y + pad, 8), :] = merged[0][p, t] - merged[1][p, t]

    def merged_rows(y, t, p, offset):
        lower = sums[0, t, p, pl.ds(y, 8), :] + diffs[0, t, p, pl.ds(y + pad - offset, 8), :]
        upper = sums[1, t, p, pl.ds(y, 8), :] + diffs[1, t, p, pl.ds(y + pad - offset, 8), :]
        return lower + upper + pltpu.roll(lower - upper, offset, 1)

    split_lanes(a0, 1, lo0, hi0, range(count), range(2, planes + 4), 1)

    def coarse_step(j, carry):
        y = pl.multiple_of(j * 8, 8)
        for t in range(2):
            v = [lo0[t, p, pl.ds(y, 8), :] + lo0[t, p, pl.ds(y + 1, 8), :] for p in range(count)]
            for p in range(count - 1):
                w = v[p] + v[p + 1]
                a1[t, p, pl.ds(y, 8), :] = w
        return carry

    lax.fori_loop(0, steps, coarse_step, 0)

    split_lanes(a1, 0, lo1, hi1, range(count - 1), range(count - 1), 2)

    def level_one(j, carry):
        detail_step(pl.multiple_of(j * 8, 8), lo1, hi1, 2, 1, 0, planes + 2, None)
        return carry

    lax.fori_loop(0, steps, level_one, 0)

    def level_one_merge(j, carry):
        y = pl.multiple_of(j * 8, 8)
        for t in range(2):
            for p in range(2, planes + 3):
                a1[t, p, pl.ds(y, 8), :] = merged_rows(y, t, p, 2) * (1.0 / 64.0)
        return carry

    lax.fori_loop(0, steps, level_one_merge, 0)

    def level_zero(j, carry):
        detail_step(pl.multiple_of(j * 8, 8), lo0, hi0, 1, 0, 2, planes + 2, a1)
        return carry

    lax.fori_loop(0, steps, level_zero, 0)

    def level_zero_merge(j, carry):
        y = pl.multiple_of(j * 8, 8)
        for t in range(2):
            for p in range(planes):
                value = a0[t, 1 + margin + p, pl.ds(y, 8), :] - merged_rows(y, t, margin + p, 1) * (1.0 / 64.0)
                mixed[t, pl.ds(y * planes + p, 8, stride=planes), :] = value
        return carry

    lax.fori_loop(0, steps, level_zero_merge, 0)
    for t in range(2):
        kept = mixed[t, edge * planes : (rows - edge) * planes].astype(out_ref.dtype)
        for copy in range(out_ref.shape[0]):
            out_ref[copy, t] = kept


def resident(array):
    return pltpu.with_memory_space_constraint(array, pltpu.VMEM)


in_place = pl.BlockSpec(memory_space=pltpu.VMEM)


def whole(array):
    shape = array.shape
    return pl.BlockSpec(shape, lambda *_: (0,) * len(shape))


def shrink(row, chip, halo, thresholds, edge, copies):
    _, chip_planes, rows, width = chip.shape
    planes = chip_planes // 2
    margin = halo.shape[1]
    count = planes + 2 * margin
    scale = np.array([[2.0 ** (1.5 * (level + 1))] for level in range(thresholds.shape[0])], np.float32)
    limits = thresholds * scale
    f32 = jnp.float32
    buffers = [
        pltpu.VMEM((2, chip_planes + planes, rows, width), f32),
        pltpu.VMEM((2, count, rows + 8, width), f32),
        pltpu.VMEM((2, count, rows + 8, width), f32),
        pltpu.VMEM((2, count, rows, width), f32),
        pltpu.VMEM((2, count, rows + 8, width), f32),
        pltpu.VMEM((2, count, rows + 8, width), f32),
        pltpu.VMEM((2, 2, count, rows, width), f32),
        pltpu.VMEM((2, 2, count, rows + 8, width), f32),
        pltpu.VMEM((2, rows * planes, width), f32),
    ]

    def kernel(*refs):
        wavelet_kernel(edge, margin, *refs)

    return pl.pallas_call(
        kernel,
        out_shape=pltpu.VMEM((copies, 2, (rows - 2 * edge) * planes, width), jnp.bfloat16),
        in_specs=[
            pl.BlockSpec(memory_space=pltpu.SMEM),
            in_place,
            in_place,
            pl.BlockSpec(memory_space=pltpu.SMEM),
        ],
        out_specs=pl.BlockSpec(memory_space=pltpu.VMEM),
        scratch_shapes=buffers,
        name="wavelet",
    )(row, resident(chip), resident(halo), limits)


def local(image, sens, measured, mask, thresholds):
    _, phase_cells, planes, width = image.shape
    coils = sens.shape[1]
    own_lines, depth_cells = measured.shape[2], measured.shape[3]
    slabs, rows, columns = (lax.axis_size(name) for name in ("slab", "row", "coil"))
    row = lax.axis_index("row")
    lines = own_lines * rows
    group = lines * planes
    half = coils // rows
    bf16, f32 = jnp.bfloat16, jnp.float32
    other = [(0, 1), (1, 0)]

    order = (np.arange(slabs)[None, :] * lines + np.arange(lines)[:, None]).reshape(-1)
    depth_order = np.arange(depth_cells).reshape(slabs, rows, planes).transpose(1, 0, 2).reshape(-1)
    table_phase = fourier_table(phase_cells, -1.0, rows=order)
    inverse_phase = fourier_table(phase_cells, 1.0, columns=order)
    table_depth = fourier_table(depth_cells, -1.0, columns=depth_order)
    inverse_depth = fourier_table(depth_cells, 1.0, rows=depth_order)
    inverse_readout = fourier_table(width, 1.0).T.reshape(2, width, 2, width)

    image_rows = image.reshape(2, phase_cells * planes, width)
    sens_rows = sens.reshape(2, coils, phase_cells * planes, width)
    sens_spec = (2, 1, phase_cells * planes, width)
    piece = (slabs, 2, half, group, width)
    exchanged = jax.ShapeDtypeStruct((slabs, rows, 2, half, group, width), bf16)
    stack = pltpu.VMEM((2, phase_cells * planes, width), f32)
    here = row.astype(jnp.int32).reshape(1)

    def given(kernel, grid_spec, out_shape, name):
        return pl.pallas_call(kernel, grid_spec=grid_spec, out_shape=out_shape, name=name)

    def send_kernel(_, *refs):
        forward_kernel(slabs, lines, planes, pl.program_id(0), *refs)

    sent = given(
        send_kernel,
        pltpu.PrefetchScalarGridSpec(
            num_scalar_prefetch=1,
            grid=(half,),
            in_specs=[
                pl.BlockSpec(sens_spec, lambda c, r: (0, (1 - r[0]) * half + c, 0, 0)),
                whole(image_rows),
                whole(table_phase),
            ],
            out_specs=in_place,
            scratch_shapes=[stack, stack],
        ),
        pltpu.VMEM(piece, bf16),
        "forward_sent",
    )(here, sens_rows, image_rows, table_phase)
    arrived = lax.ppermute(sent, "row", other)

    def keep_kernel(_, sens_ref, image_ref, table_ref, out_ref, product, mixed):
        forward_kernel(slabs, lines, planes, 0, sens_ref, image_ref, table_ref, out_ref.at[:, 0], product, mixed)

    kept = given(
        keep_kernel,
        pltpu.PrefetchScalarGridSpec(
            num_scalar_prefetch=1,
            grid=(half,),
            in_specs=[
                pl.BlockSpec(sens_spec, lambda c, r: (0, r[0] * half + c, 0, 0)),
                whole(image_rows),
                whole(table_phase),
            ],
            out_specs=pl.BlockSpec((slabs, 1, 2, 1, group, width), lambda c, r: (0, 0, 0, c, 0, 0)),
            scratch_shapes=[stack, stack],
        ),
        exchanged,
        "forward_kept",
    )(here, sens_rows, image_rows, table_phase)

    def place_kernel(r_ref, _, arrived_ref, out_ref, pause_ref, done):
        copy = pltpu.make_async_copy(arrived_ref, out_ref.at[:, 1], done)
        copy.start()
        pause_ref[...] = lax.fori_loop(
            0, r_ref[0] * pause_steps, lambda _, v: v * 1.0001 + 0.5, jnp.ones(pause_ref.shape, jnp.float32)
        )
        copy.wait()

    outgoing, _ = pl.pallas_call(
        place_kernel,
        in_specs=[
            pl.BlockSpec(memory_space=pltpu.SMEM),
            pl.BlockSpec(memory_space=pl.ANY),
            in_place,
        ],
        out_specs=[pl.BlockSpec(memory_space=pl.ANY), pl.BlockSpec(memory_space=pltpu.VMEM)],
        out_shape=[exchanged, jax.ShapeDtypeStruct((8, 128), f32)],
        scratch_shapes=[pltpu.SemaphoreType.DMA],
        input_output_aliases={1: 0},
        name="place",
    )(here, kept, resident(arrived))

    received = lax.all_to_all(outgoing, "slab", 0, 0, tiled=True)

    measured, mask, sens_late, image, _ = lax.optimization_barrier((measured, mask, sens_rows, image, outgoing))

    def both_rows(values, axis):
        kept = lax.dynamic_slice_in_dim(values, row * half, half, axis=1)
        away = lax.dynamic_slice_in_dim(values, (1 - row) * half, half, axis=1)
        return in_row_order(kept, lax.ppermute(away, "row", other), axis)

    def in_row_order(own, others, axis):
        first = row == 0
        return jnp.concatenate([jnp.where(first, own, others), jnp.where(first, others, own)], axis=axis)

    own_measured = jnp.einsum(
        "tclzk,tksx->sclzx", measured, inverse_readout, preferred_element_type=f32
    ).astype(bf16)
    chip_measured = both_rows(own_measured, 2)
    own_mask = mask.astype(f32)
    chip_mask = in_row_order(own_mask, lax.ppermute(own_mask, "row", other), 0)
    wide_mask = jnp.broadcast_to(chip_mask[:, :, None], (lines, depth_cells, width))
    chip_sens = both_rows(sens_late[:, :, None], 2)
    edge = 4
    quarter = phase_cells // columns
    image_planes = jnp.transpose(image, (0, 2, 1, 3))
    framed = jnp.concatenate(
        [image_planes[:, :, phase_cells - edge :], image_planes, image_planes[:, :, :edge]], axis=2
    )
    own_image = lax.dynamic_slice_in_dim(
        framed, lax.axis_index("coil") * quarter, quarter + 2 * edge, axis=2
    )
    chip_image = in_row_order(own_image, lax.ppermute(own_image, "row", other), 1)

    def mid_kernel(*refs):
        middle_kernel(lines, *refs)

    buffer = pltpu.VMEM((rows, 2, slabs * group, width), f32)
    returning = given(
        mid_kernel,
        pltpu.PrefetchScalarGridSpec(
            num_scalar_prefetch=1,
            grid=(half,),
            in_specs=[
                in_place,
                in_place,
                in_place,
                whole(table_depth),
                whole(inverse_depth),
            ],
            out_specs=pl.BlockSpec((slabs, rows, 2, 1, group, width), lambda c, r: (0, 0, 0, c, 0, 0)),
            scratch_shapes=[buffer, buffer],
        ),
        exchanged,
        "middle",
    )(here, *map(resident, (received, chip_measured, wide_mask)), table_depth, inverse_depth)
    returned = lax.all_to_all(returning, "slab", 0, 0, tiled=True)
    margin = 2 ** thresholds.shape[0] - 1
    around = []
    for slab in range(slabs):
        after = (slab + 1) % slabs
        around += [(slab * rows + rows - 1, after * rows), (after * rows, slab * rows + rows - 1)]
    border = jnp.where(row == 0, own_image[:, :margin], own_image[:, planes - margin :])
    halo_image = lax.ppermute(border, lines_axes, around)
    returned, chip_image, halo_image = lax.optimization_barrier((returned, chip_image, halo_image))

    tall = quarter + 2 * edge

    def back_kernel(*refs):
        backward_kernel(lines, planes, edge, *refs)

    parts = pl.pallas_call(
        back_kernel,
        grid=(half,),
        out_shape=pltpu.VMEM((columns, 2, rows * planes, tall, width), bf16),
        in_specs=[in_place, in_place, whole(inverse_phase)],
        out_specs=in_place,
        scratch_shapes=[
            buffer,
            buffer,
            pltpu.VMEM((rows, 2, planes, phase_cells, width), f32),
            pltpu.VMEM((phase_cells + 2 * edge, width), f32),
        ],
        name="backward",
    )(resident(returned), resident(chip_sens), inverse_phase)
    share = lax.all_to_all(parts, "coil", 0, 0, tiled=True).astype(f32).sum(axis=0)
    narrow = share.astype(bf16)
    margin = 2 ** thresholds.shape[0] - 1
    last = rows * planes - margin
    same, across = [], []
    for slab in range(slabs):
        after = (slab + 1) % slabs
        same += [(slab * rows, after * rows), (after * rows + rows - 1, slab * rows + rows - 1)]
        across += [(slab * rows + rows - 1, after * rows), (after * rows, slab * rows + rows - 1)]
    low_planes, high_planes = narrow[:, :margin], narrow[:, last:]
    first = row == 0
    to_same = jnp.where(first, high_planes, low_planes)
    to_across = jnp.where(first, low_planes, high_planes)
    others = lax.ppermute(narrow, "row", other)
    halo_same = lax.ppermute(to_same, lines_axes, same)
    halo_across = lax.ppermute(to_across, lines_axes, across)
    chip = chip_image - step_size * (share + others.astype(f32))
    halo = halo_image - step_size * (halo_same.astype(f32) + halo_across.astype(f32))
    result = shrink(here, chip, halo, thresholds, edge, columns)
    gathered = lax.all_to_all(result, "coil", 0, 0, tiled=True)
    result_rows = jnp.swapaxes(gathered, 0, 1).reshape(2, phase_cells * planes, width)
    return result_rows.astype(f32).reshape(2, phase_cells, planes, width)


def solution(mesh):
    return jax.shard_map(
        local,
        mesh=mesh,
        in_specs=(
            P("groups", None, lines_axes, None),
            P("groups", "coil", None, lines_axes, None),
            P("groups", "coil", lines_axes, None, None),
            P(lines_axes, None),
            P(),
        ),
        out_specs=P("groups", None, lines_axes, None),
        check_vma=False,
    )
```

```python
import math

import jax
import jax.numpy as jnp
import ml_dtypes
import numpy as np
from jax import lax
from jax.experimental import pallas as pl
from jax.experimental.pallas import tpu as pltpu
from jax.sharding import PartitionSpec as P

step_size = 0.5
lines_axes = ("slab", "row")
pause_steps = 7100


def fourier_table(length, sign, rows=None, columns=None):
    index = np.arange(length, dtype=np.int64)
    phase = (index[:, None] * index[None, :]) % length
    theta = phase.astype(np.float32) * np.float32(2.0 * math.pi / length)
    scale = np.float32(1.0 / math.sqrt(length))
    real = (np.cos(theta) * scale).astype(np.float32)
    imaginary = (np.sin(theta) * np.float32(sign) * scale).astype(np.float32)
    if rows is not None:
        real, imaginary = real[rows], imaginary[rows]
    if columns is not None:
        real, imaginary = real[:, columns], imaginary[:, columns]
    return np.block([[real, -imaginary], [imaginary, real]]).astype(ml_dtypes.bfloat16)


def dot(left, right):
    return jnp.dot(left, right, preferred_element_type=jnp.float32)


def forward_kernel(slabs, lines, planes, coil, sens_ref, image_ref, table_ref, out_ref, product, mixed):
    cells = product.shape[1] // planes
    group = lines * planes
    sr = sens_ref[0, 0].astype(jnp.float32)
    si = sens_ref[1, 0].astype(jnp.float32)
    ir = image_ref[0]
    ii = image_ref[1]
    product[0] = sr * ir - si * ii
    product[1] = sr * ii + si * ir
    columns = [
        jnp.concatenate(
            [product[t, pl.ds(z, cells, stride=planes), :].astype(jnp.bfloat16) for t in range(2)],
            axis=0,
        )
        for z in range(planes)
    ]
    done = dot(table_ref[...], jnp.concatenate(columns, axis=1))
    width = product.shape[2]
    for s in range(2):
        for z in range(planes):
            for line in range(lines):
                first = s * cells + line * slabs
                mixed[s, pl.ds(z * lines + line, slabs, stride=group), :] = done[
                    first : first + slabs, z * width : (z + 1) * width
                ]
        out_ref[:, s, coil] = mixed[s].astype(jnp.bfloat16).reshape(slabs, group, width)


def middle_kernel(lines, row_ref, in_ref, measured_ref, mask_ref, table_ref, inverse_ref, out_ref, mixed, back):
    slabs, _, _, _, group, width = in_ref.shape
    half = slabs * group // lines
    cells = 2 * half
    coil = pl.program_id(0)
    for row in range(2):
        place = row_ref[0] if row == 0 else 1 - row_ref[0]
        for t in range(2):
            mixed[row, t] = in_ref[:, place, t, coil].astype(jnp.float32).reshape(slabs * group, width)
    columns = [
        jnp.concatenate(
            [
                mixed[row, t, pl.ds(line, half, stride=lines), :].astype(jnp.bfloat16)
                for t in range(2)
                for row in range(2)
            ],
            axis=0,
        )
        for line in range(lines)
    ]
    spectrum = dot(table_ref[...], jnp.concatenate(columns, axis=1))
    residual = []
    for line in range(lines):
        parts = []
        for t in range(2):
            value = spectrum[t * cells : (t + 1) * cells, line * width : (line + 1) * width]
            value = mask_ref[line] * (value - measured_ref[t, coil, line].astype(jnp.float32))
            parts.append(value.astype(jnp.bfloat16))
        residual.append(jnp.concatenate(parts, axis=0))
    result = dot(inverse_ref[...], jnp.concatenate(residual, axis=1))
    for row in range(2):
        for s in range(2):
            first = s * cells + row * half
            for line in range(lines):
                back[row, s, pl.ds(line, half, stride=lines), :] = result[
                    first : first + half, line * width : (line + 1) * width
                ]
            out_ref[:, row, s, 0] = back[row, s].astype(jnp.bfloat16).reshape(slabs, group, width)


def backward_kernel(lines, planes, edge, in_ref, sens_ref, table_ref, out_ref, mixed, wide, total, framed):
    slabs, rows, _, _, group, width = in_ref.shape
    cells = slabs * lines
    coil = pl.program_id(0)

    @pl.when(coil == 0)
    def _():
        total[...] = jnp.zeros(total.shape, jnp.float32)

    for row in range(rows):
        for t in range(2):
            mixed[row, t] = in_ref[:, row, t, coil].astype(jnp.float32).reshape(slabs * group, width)
            wide[row, t] = sens_ref[t, coil, row].astype(jnp.float32)
    columns = [
        jnp.concatenate(
            [
                mixed[row, t, pl.ds(z * lines + line, slabs, stride=group), :].astype(jnp.bfloat16)
                for t in range(2)
                for line in range(lines)
            ],
            axis=0,
        )
        for row in range(rows)
        for z in range(planes)
    ]
    done = dot(table_ref[...], jnp.concatenate(columns, axis=1))
    for row in range(rows):
        for z in range(planes):
            plane = row * planes + z
            rr = done[:cells, plane * width : (plane + 1) * width]
            ri = done[cells:, plane * width : (plane + 1) * width]
            sr = wide[row, 0, pl.ds(z, cells, stride=planes), :]
            si = wide[row, 1, pl.ds(z, cells, stride=planes), :]
            total[row, 0, z] += sr * rr + si * ri
            total[row, 1, z] += sr * ri - si * rr

    @pl.when(coil == pl.num_programs(0) - 1)
    def _():
        pieces, _, _, tall, _ = out_ref.shape
        step = tall - 2 * edge
        for row in range(rows):
            for t in range(2):
                for z in range(planes):
                    framed[0:edge] = total[row, t, z, cells - edge : cells]
                    framed[edge : edge + cells] = total[row, t, z]
                    framed[edge + cells :] = total[row, t, z, 0:edge]
                    for q in range(pieces):
                        out_ref[q, t, row * planes + z] = framed[q * step : q * step + tall].astype(out_ref.dtype)


def removed(real, imaginary, limit):
    factor = jnp.minimum(lax.rsqrt(real * real + imaginary * imaginary) * limit, 1.0)
    return real * factor, imaginary * factor


def wavelet_kernel(edge, margin, row_ref, chip_ref, halo_ref, limits_ref, out_ref, a0, lo0, hi0, a1, lo1, hi1, sums, diffs, mixed):
    chip_planes, rows, width = chip_ref.shape[1:]
    planes = chip_planes // 2
    count = planes + 2 * margin
    steps = rows // 8
    pad = 8
    row = row_ref[0]
    for t in range(2):
        for p in range(chip_planes):
            a0[t, (1 - row) * planes + p] = chip_ref[t, p]
        for p in range(margin):
            a0[t, 1 + row * (margin + planes) + p] = halo_ref[t, p].astype(jnp.float32)

    def split_lanes(source, shift, lo, hi, lo_planes, hi_planes, offset):
        def step(j, carry):
            y = pl.multiple_of(j * 8, 8)
            for t in range(2):
                for p in lo_planes:
                    v = source[t, p + shift, pl.ds(y, 8), :]
                    s = pltpu.roll(v, width - offset, 1)
                    lo[t, p, pl.ds(y, 8), :] = v + s
                    if p in hi_planes:
                        hi[t, p, pl.ds(y, 8), :] = v - s
            return carry

        lax.fori_loop(0, steps, step, 0)

    def detail_step(y, lo, hi, offset, level, first, last, coarse):
        for x_band, source in ((0, lo), (1, hi)):
            merged = []
            for y_band in range(2):
                band = x_band + 2 * y_band
                v = {}
                for p in range(first, last + offset + 1):
                    for t in range(2):
                        here = source[t, p, pl.ds(y, 8), :]
                        there = source[t, p, pl.ds(y + offset, 8), :]
                        v[p, t] = here + there if y_band == 0 else here - there
                plus, minus = {}, {}
                for p in range(first, last + 1):
                    high = removed(
                        v[p, 0] - v[p + offset, 0], v[p, 1] - v[p + offset, 1], limits_ref[level, band + 3]
                    )
                    if band:
                        low = removed(
                            v[p, 0] + v[p + offset, 0], v[p, 1] + v[p + offset, 1], limits_ref[level, band - 1]
                        )
                    elif coarse is not None:
                        low = (coarse[0, p, pl.ds(y, 8), :], coarse[1, p, pl.ds(y, 8), :])
                    else:
                        low = None
                    for t in range(2):
                        plus[p, t] = high[t] if low is None else low[t] + high[t]
                        minus[p, t] = -high[t] if low is None else low[t] - high[t]
                merged.append(
                    {
                        (p, t): plus[p, t] + minus[p - offset, t]
                        for p in range(first + offset, last + 1)
                        for t in range(2)
                    }
                )
            for p, t in merged[0]:
                sums[x_band, t, p, pl.ds(y, 8), :] = merged[0][p, t] + merged[1][p, t]
                diffs[x_band, t, p, pl.ds(y + pad, 8), :] = merged[0][p, t] - merged[1][p, t]

    def merged_rows(y, t, p, offset):
        lower = sums[0, t, p, pl.ds(y, 8), :] + diffs[0, t, p, pl.ds(y + pad - offset, 8), :]
        upper = sums[1, t, p, pl.ds(y, 8), :] + diffs[1, t, p, pl.ds(y + pad - offset, 8), :]
        return lower + upper + pltpu.roll(lower - upper, offset, 1)

    split_lanes(a0, 1, lo0, hi0, range(count), range(2, planes + 4), 1)

    def coarse_step(j, carry):
        y = pl.multiple_of(j * 8, 8)
        for t in range(2):
            v = [lo0[t, p, pl.ds(y, 8), :] + lo0[t, p, pl.ds(y + 1, 8), :] for p in range(count)]
            for p in range(count - 1):
                w = v[p] + v[p + 1]
                a1[t, p, pl.ds(y, 8), :] = w
        return carry

    lax.fori_loop(0, steps, coarse_step, 0)

    split_lanes(a1, 0, lo1, hi1, range(count - 1), range(count - 1), 2)

    def level_one(j, carry):
        detail_step(pl.multiple_of(j * 8, 8), lo1, hi1, 2, 1, 0, planes + 2, None)
        return carry

    lax.fori_loop(0, steps, level_one, 0)

    def level_one_merge(j, carry):
        y = pl.multiple_of(j * 8, 8)
        for t in range(2):
            for p in range(2, planes + 3):
                a1[t, p, pl.ds(y, 8), :] = merged_rows(y, t, p, 2) * (1.0 / 64.0)
        return carry

    lax.fori_loop(0, steps, level_one_merge, 0)

    def level_zero(j, carry):
        detail_step(pl.multiple_of(j * 8, 8), lo0, hi0, 1, 0, 2, planes + 2, a1)
        return carry

    lax.fori_loop(0, steps, level_zero, 0)

    def level_zero_merge(j, carry):
        y = pl.multiple_of(j * 8, 8)
        for t in range(2):
            for p in range(planes):
                value = a0[t, 1 + margin + p, pl.ds(y, 8), :] - merged_rows(y, t, margin + p, 1) * (1.0 / 64.0)
                mixed[t, pl.ds(y * planes + p, 8, stride=planes), :] = value
        return carry

    lax.fori_loop(0, steps, level_zero_merge, 0)
    for t in range(2):
        kept = mixed[t, edge * planes : (rows - edge) * planes].astype(out_ref.dtype)
        for copy in range(out_ref.shape[0]):
            out_ref[copy, t] = kept


def resident(array):
    return pltpu.with_memory_space_constraint(array, pltpu.VMEM)


in_place = pl.BlockSpec(memory_space=pltpu.VMEM)


def whole(array):
    shape = array.shape
    return pl.BlockSpec(shape, lambda *_: (0,) * len(shape))


def shrink(row, chip, halo, thresholds, edge, copies):
    _, chip_planes, rows, width = chip.shape
    planes = chip_planes // 2
    margin = halo.shape[1]
    count = planes + 2 * margin
    scale = np.array([[2.0 ** (1.5 * (level + 1))] for level in range(thresholds.shape[0])], np.float32)
    limits = thresholds * scale
    f32 = jnp.float32
    buffers = [
        pltpu.VMEM((2, chip_planes + planes, rows, width), f32),
        pltpu.VMEM((2, count, rows + 8, width), f32),
        pltpu.VMEM((2, count, rows + 8, width), f32),
        pltpu.VMEM((2, count, rows, width), f32),
        pltpu.VMEM((2, count, rows + 8, width), f32),
        pltpu.VMEM((2, count, rows + 8, width), f32),
        pltpu.VMEM((2, 2, count, rows, width), f32),
        pltpu.VMEM((2, 2, count, rows + 8, width), f32),
        pltpu.VMEM((2, rows * planes, width), f32),
    ]

    def kernel(*refs):
        wavelet_kernel(edge, margin, *refs)

    return pl.pallas_call(
        kernel,
        out_shape=pltpu.VMEM((copies, 2, (rows - 2 * edge) * planes, width), jnp.bfloat16),
        in_specs=[
            pl.BlockSpec(memory_space=pltpu.SMEM),
            in_place,
            in_place,
            pl.BlockSpec(memory_space=pltpu.SMEM),
        ],
        out_specs=pl.BlockSpec(memory_space=pltpu.VMEM),
        scratch_shapes=buffers,
        name="wavelet",
    )(row, resident(chip), resident(halo), limits)


def local(image, sens, measured, mask, thresholds):
    _, phase_cells, planes, width = image.shape
    coils = sens.shape[1]
    own_lines, depth_cells = measured.shape[2], measured.shape[3]
    slabs, rows, columns = (lax.axis_size(name) for name in ("slab", "row", "coil"))
    row = lax.axis_index("row")
    lines = own_lines * rows
    group = lines * planes
    half = coils // rows
    bf16, f32 = jnp.bfloat16, jnp.float32
    other = [(0, 1), (1, 0)]

    order = (np.arange(slabs)[None, :] * lines + np.arange(lines)[:, None]).reshape(-1)
    depth_order = np.arange(depth_cells).reshape(slabs, rows, planes).transpose(1, 0, 2).reshape(-1)
    table_phase = fourier_table(phase_cells, -1.0, rows=order)
    inverse_phase = fourier_table(phase_cells, 1.0, columns=order)
    table_depth = fourier_table(depth_cells, -1.0, columns=depth_order)
    inverse_depth = fourier_table(depth_cells, 1.0, rows=depth_order)
    inverse_readout = fourier_table(width, 1.0).T.reshape(2, width, 2, width)

    image_rows = image.reshape(2, phase_cells * planes, width)
    sens_rows = sens.reshape(2, coils, phase_cells * planes, width)
    sens_spec = (2, 1, phase_cells * planes, width)
    piece = (slabs, 2, half, group, width)
    exchanged = jax.ShapeDtypeStruct((slabs, rows, 2, half, group, width), bf16)
    stack = pltpu.VMEM((2, phase_cells * planes, width), f32)
    here = row.astype(jnp.int32).reshape(1)

    def given(kernel, grid_spec, out_shape, name):
        return pl.pallas_call(kernel, grid_spec=grid_spec, out_shape=out_shape, name=name)

    def send_kernel(_, *refs):
        forward_kernel(slabs, lines, planes, pl.program_id(0), *refs)

    sent = given(
        send_kernel,
        pltpu.PrefetchScalarGridSpec(
            num_scalar_prefetch=1,
            grid=(half,),
            in_specs=[
                pl.BlockSpec(sens_spec, lambda c, r: (0, (1 - r[0]) * half + c, 0, 0)),
                whole(image_rows),
                whole(table_phase),
            ],
            out_specs=in_place,
            scratch_shapes=[stack, stack],
        ),
        pltpu.VMEM(piece, bf16),
        "forward_sent",
    )(here, sens_rows, image_rows, table_phase)
    arrived = lax.ppermute(sent, "row", other)

    def keep_kernel(_, sens_ref, image_ref, table_ref, out_ref, product, mixed):
        forward_kernel(slabs, lines, planes, 0, sens_ref, image_ref, table_ref, out_ref.at[:, 0], product, mixed)

    kept = given(
        keep_kernel,
        pltpu.PrefetchScalarGridSpec(
            num_scalar_prefetch=1,
            grid=(half,),
            in_specs=[
                pl.BlockSpec(sens_spec, lambda c, r: (0, r[0] * half + c, 0, 0)),
                whole(image_rows),
                whole(table_phase),
            ],
            out_specs=pl.BlockSpec((slabs, 1, 2, 1, group, width), lambda c, r: (0, 0, 0, c, 0, 0)),
            scratch_shapes=[stack, stack],
        ),
        exchanged,
        "forward_kept",
    )(here, sens_rows, image_rows, table_phase)

    def place_kernel(r_ref, _, arrived_ref, out_ref, pause_ref, done):
        copy = pltpu.make_async_copy(arrived_ref, out_ref.at[:, 1], done)
        copy.start()
        pause_ref[...] = lax.fori_loop(
            0, r_ref[0] * pause_steps, lambda _, v: v * 1.0001 + 0.5, jnp.ones(pause_ref.shape, jnp.float32)
        )
        copy.wait()

    outgoing, _ = pl.pallas_call(
        place_kernel,
        in_specs=[
            pl.BlockSpec(memory_space=pltpu.SMEM),
            pl.BlockSpec(memory_space=pl.ANY),
            in_place,
        ],
        out_specs=[pl.BlockSpec(memory_space=pl.ANY), pl.BlockSpec(memory_space=pltpu.VMEM)],
        out_shape=[exchanged, jax.ShapeDtypeStruct((8, 128), f32)],
        scratch_shapes=[pltpu.SemaphoreType.DMA],
        input_output_aliases={1: 0},
        name="place",
    )(here, kept, resident(arrived))

    received = lax.all_to_all(outgoing, "slab", 0, 0, tiled=True)

    measured, mask, sens_late, image, _ = lax.optimization_barrier((measured, mask, sens_rows, image, outgoing))

    def both_rows(values, axis):
        kept = lax.dynamic_slice_in_dim(values, row * half, half, axis=1)
        away = lax.dynamic_slice_in_dim(values, (1 - row) * half, half, axis=1)
        return in_row_order(kept, lax.ppermute(away, "row", other), axis)

    def in_row_order(own, others, axis):
        first = row == 0
        return jnp.concatenate([jnp.where(first, own, others), jnp.where(first, others, own)], axis=axis)

    own_measured = jnp.einsum(
        "tclzk,tksx->sclzx", measured, inverse_readout, preferred_element_type=f32
    ).astype(bf16)
    chip_measured = both_rows(own_measured, 2)
    own_mask = mask.astype(f32)
    chip_mask = in_row_order(own_mask, lax.ppermute(own_mask, "row", other), 0)
    wide_mask = jnp.broadcast_to(chip_mask[:, :, None], (lines, depth_cells, width))
    chip_sens = both_rows(sens_late[:, :, None], 2)
    edge = 4
    quarter = phase_cells // columns
    image_planes = jnp.transpose(image, (0, 2, 1, 3))
    framed = jnp.concatenate(
        [image_planes[:, :, phase_cells - edge :], image_planes, image_planes[:, :, :edge]], axis=2
    )
    own_image = lax.dynamic_slice_in_dim(
        framed, lax.axis_index("coil") * quarter, quarter + 2 * edge, axis=2
    )
    chip_image = in_row_order(own_image, lax.ppermute(own_image, "row", other), 1)

    def mid_kernel(*refs):
        middle_kernel(lines, *refs)

    buffer = pltpu.VMEM((rows, 2, slabs * group, width), f32)
    returning = given(
        mid_kernel,
        pltpu.PrefetchScalarGridSpec(
            num_scalar_prefetch=1,
            grid=(half,),
            in_specs=[
                in_place,
                in_place,
                in_place,
                whole(table_depth),
                whole(inverse_depth),
            ],
            out_specs=pl.BlockSpec((slabs, rows, 2, 1, group, width), lambda c, r: (0, 0, 0, c, 0, 0)),
            scratch_shapes=[buffer, buffer],
        ),
        exchanged,
        "middle",
    )(here, *map(resident, (received, chip_measured, wide_mask)), table_depth, inverse_depth)
    returned = lax.all_to_all(returning, "slab", 0, 0, tiled=True)
    returned, chip_image = lax.optimization_barrier((returned, chip_image))

    tall = quarter + 2 * edge

    def back_kernel(*refs):
        backward_kernel(lines, planes, edge, *refs)

    parts = pl.pallas_call(
        back_kernel,
        grid=(half,),
        out_shape=pltpu.VMEM((columns, 2, rows * planes, tall, width), bf16),
        in_specs=[in_place, in_place, whole(inverse_phase)],
        out_specs=in_place,
        scratch_shapes=[
            buffer,
            buffer,
            pltpu.VMEM((rows, 2, planes, phase_cells, width), f32),
            pltpu.VMEM((phase_cells + 2 * edge, width), f32),
        ],
        name="backward",
    )(resident(returned), resident(chip_sens), inverse_phase)
    share = lax.all_to_all(parts, "coil", 0, 0, tiled=True).astype(f32).sum(axis=0)
    others = lax.ppermute(share.astype(bf16), "row", other)
    chip = chip_image - step_size * (share + others.astype(f32))
    margin = 2 ** thresholds.shape[0] - 1
    last = rows * planes - margin
    edge_planes = lax.dynamic_slice_in_dim(chip, row * last, margin, axis=1).astype(bf16)
    pairs = []
    for slab in range(slabs):
        after = (slab + 1) % slabs
        pairs.append((slab * rows + rows - 1, after * rows))
        pairs.append((after * rows, slab * rows + rows - 1))
    halo = lax.ppermute(edge_planes, lines_axes, pairs)
    result = shrink(here, chip, halo, thresholds, edge, columns)
    gathered = lax.all_to_all(result, "coil", 0, 0, tiled=True)
    result_rows = jnp.swapaxes(gathered, 0, 1).reshape(2, phase_cells * planes, width)
    return result_rows.astype(f32).reshape(2, phase_cells, planes, width)


def solution(mesh):
    return jax.shard_map(
        local,
        mesh=mesh,
        in_specs=(
            P("groups", None, lines_axes, None),
            P("groups", "coil", None, lines_axes, None),
            P("groups", "coil", lines_axes, None, None),
            P(lines_axes, None),
            P(),
        ),
        out_specs=P("groups", None, lines_axes, None),
        check_vma=False,
    )
```
